128 devices in a mesh: f: 16 (over z, y), h: 8 (over x, core).
Axes of the slice: x: 4, y: 4, z: 4, core: 2. Of those that a mesh axis runs over, the one named last changes fastest.
Arguments:
- x: bfloat16 [4096, 3072], P(None, 'h')
- g1: float32 [3072], P('h')
- g2: float32 [3072], P('h')
- w_gate: bfloat16 [3072, 24576], P('h', 'f')
- w_up: bfloat16 [3072, 24576], P('h', 'f')
- w_down: bfloat16 [24576, 3072], P('f', 'h')
- o: bfloat16 [4096, 4096], P(None, 'f')
- w_o: bfloat16 [4096, 3072], P('f', 'h')
- w_qkv: bfloat16 [3072, 12288], P('h', 'f')
Outputs:
- output 1: bfloat16 [4096, 3072], P(None, 'h')
- output 2: bfloat16 [4096, 12288], P(None, 'f')
All inputs are finite; a program needn't handle non-finite values.
Results may differ from the reference program's by a relative error of at most 0.0040629.
Values are sent between devices in bfloat16 or wider.
A program may use at most 1 GiB of HBM per device.

```python
import jax
import jax.numpy as jnp
from jax import lax

T = 4096
D = 3072
FF = 24576
HEADS = 16
KV_HEADS = 16
HEAD = 256
HD = HEADS * HEAD
Q = (HEADS + 2 * KV_HEADS) * HEAD
EPS = 1e-6


def _w(key, shape):
    return (jax.random.normal(key, shape, jnp.float32) * shape[0] ** -0.5).astype(jnp.bfloat16)


def setup_inputs(seed: int = 0) -> dict:
    ks = jax.random.split(jax.random.PRNGKey(seed), 11)
    z = jax.random.normal(ks[0], (T, D), jnp.float32)
    row = jnp.exp(jax.random.uniform(ks[1], (T, 1), jnp.float32, -1.0, 1.0))
    tilt = jax.random.uniform(ks[2], (T, 1), jnp.float32, -1.0, 1.0)
    pos = jnp.arange(D, dtype=jnp.float32)[None, :] * (2.0 / D) - 1.0
    x = (z * row * jnp.exp(tilt * pos)).astype(jnp.bfloat16)
    o = (0.7 * jax.random.normal(ks[8], (T, HD), jnp.float32)).astype(jnp.bfloat16)
    return {
        'x': x,
        'g1': jax.random.uniform(ks[3], (D,), jnp.float32, 0.5, 1.5),
        'g2': jax.random.uniform(ks[4], (D,), jnp.float32, 0.5, 1.5),
        'w_gate': _w(ks[5], (D, FF)),
        'w_up': _w(ks[6], (D, FF)),
        'w_down': _w(ks[7], (FF, D)),
        'o': o,
        'w_o': _w(ks[9], (HD, D)),
        'w_qkv': _w(ks[10], (D, Q)),
    }


def _norm(x, g):
    xf = x.astype(jnp.float32)
    r = lax.rsqrt(jnp.mean(xf * xf, axis=-1, keepdims=True) + EPS)
    return (xf * r * g).astype(jnp.bfloat16)


def reference(x, g1, g2, w_gate, w_up, w_down, o, w_o, w_qkv):
    n = _norm(x, g1)
    gt = jnp.dot(n, w_gate, preferred_element_type=jnp.float32)
    up = jnp.dot(n, w_up, preferred_element_type=jnp.float32)
    a = (jax.nn.silu(gt) * up).astype(jnp.bfloat16)
    y = jnp.dot(a, w_down, preferred_element_type=jnp.float32) + jnp.dot(o, w_o, preferred_element_type=jnp.float32)
    x_next = (x.astype(jnp.float32) + y).astype(jnp.bfloat16)
    n1 = _norm(x_next, g2)
    qkv = jnp.dot(n1, w_qkv, preferred_element_type=jnp.float32).astype(jnp.bfloat16)
    return (x_next, qkv)
```

```python
import jax
import jax.numpy as jnp
from jax import lax
from jax.sharding import PartitionSpec as P

EPS = 1e-6


def _dot(a, b):
    return jnp.dot(a, b, preferred_element_type=jnp.float32)


def _norm(xf, g):
    r = lax.rsqrt(jnp.mean(xf * xf, axis=-1, keepdims=True) + EPS)
    return (xf * r * g).astype(jnp.bfloat16)


def solution(mesh):
    nh = mesh.shape['h']
    nf = mesh.shape['f']

    def body(x, g1, g2, w_gate, w_up, w_down, o, w_o, w_qkv):
        t, dh = x.shape
        th = t // nh
        tb = th // nf
        d = dh * nh
        ih = lax.axis_index('h')
        i_f = lax.axis_index('f')

        def gather_h(w, axis):
            return lax.all_gather(w, 'h', axis=axis, tiled=True)

        xs = lax.dynamic_slice(x.reshape(nh, nf, tb, dh), (0, i_f, 0, 0), (nh, 1, tb, dh))
        xs = xs.reshape(nh, tb, dh)
        xs = lax.all_to_all(xs, 'h', split_axis=0, concat_axis=0, tiled=True)
        g = lax.all_gather(jnp.stack([g1, g2]), 'h', axis=1, tiled=True)
        xs = xs.transpose(1, 0, 2).reshape(tb, d)
        xf = xs.astype(jnp.float32)
        n = lax.all_gather(_norm(xf, g[0]), 'f', axis=0, tiled=True)
        wg = gather_h(w_gate, 0)
        wu = gather_h(w_up, 0)
        a = (jax.nn.silu(_dot(n, wg)) * _dot(n, wu)).astype(jnp.bfloat16)
        wd = gather_h(w_down, 1)
        wo = gather_h(w_o, 1)
        ot = lax.dynamic_slice(o, (ih * th, 0), (th, o.shape[1]))
        y = _dot(a, wd) + _dot(ot, wo)
        y = lax.psum_scatter(y, 'f', scatter_dimension=0, tiled=True)
        xn = (xf + y).astype(jnp.bfloat16)
        n1 = lax.all_gather(_norm(xn.astype(jnp.float32), g[1]), 'f', axis=0, tiled=True)
        xo = xn.reshape(tb, nh, dh).transpose(1, 0, 2)
        xo = lax.all_to_all(xo, 'h', split_axis=0, concat_axis=0, tiled=True)
        xo = lax.all_gather(xo, 'f', axis=0, tiled=False)
        x_next = xo.transpose(1, 0, 2, 3).reshape(t, dh)
        wqkv = gather_h(w_qkv, 0)
        qkv = _dot(n1, wqkv).astype(jnp.bfloat16)
        qkv = lax.all_gather(qkv, 'h', axis=0, tiled=True)
        return x_next, qkv

    in_specs = (P(None, 'h'), P('h'), P('h'), P('h', 'f'), P('h', 'f'), P('f', 'h'),
                P(None, 'f'), P('f', 'h'), P('h', 'f'))
    return jax.shard_map(body, mesh=mesh, in_specs=in_specs,
                         out_specs=(P(None, 'h'), P(None, 'f')), check_vma=False)
```

```python
import functools

import jax
import jax.numpy as jnp
from jax import lax
from jax.experimental import pallas as pl
from jax.experimental.pallas import tpu as pltpu
from jax.sharding import PartitionSpec as P

EPS = 1e-6
MESH = pl.DeviceIdType.MESH
ANY = pl.BlockSpec(memory_space=pl.ANY)
VM = pl.BlockSpec(memory_space=pltpu.VMEM)
BF = jnp.bfloat16
F32 = jnp.float32


def _dot(a, b):
    return jnp.dot(a, b, preferred_element_type=jnp.float32)


class Pos:
    def __init__(self):
        self.f = lax.axis_index('f')
        self.h = lax.axis_index('h')
        self.z, self.y = self.f // 4, self.f % 4
        self.x, self.c = self.h // 2, self.h % 2
        self.j = self.x // 2
        self.q = quarter(self.h)
        ax = self.x + 1 - 2 * (self.x % 2)
        self.A = (self.f, 2 * ax + self.c)
        self.B = (self.f, 2 * (3 - self.x) + self.c)
        self.C = (self.f, self.h + 1 - 2 * self.c)
        self.AC = (self.f, 2 * ax + 1 - self.c)

    def H(self, d):
        return (self.f, (self.h + d) % 8)

    def Y(self, d):
        return (4 * self.z + (self.y + d) % 4, self.h)

    def Z(self, d):
        return (4 * ((self.z + d) % 4) + self.y, self.h)


def quarter(h):
    x = h // 2
    return 2 * ((x + x // 2) % 2) + h % 2


class Comm:
    def __init__(self, ssem, rsem, lsem):
        self.ssem, self.rsem, self.lsem = ssem, rsem, lsem
        self.k = 0
        self.lk = 0
        self.sent = []

    def send(self, src, dst, dev):
        c = pltpu.make_async_remote_copy(src_ref=src, dst_ref=dst, send_sem=self.ssem.at[self.k],
                                         recv_sem=self.rsem.at[self.k], device_id=dev, device_id_type=MESH)
        self.k += 1
        c.start()
        self.sent.append(c)
        return c

    def local(self, src, dst):
        c = pltpu.make_async_copy(src, dst, self.lsem.at[self.lk])
        self.lk += 1
        c.start()
        return c

    def finish(self):
        for c in self.sent:
            c.wait_send()


def barrier(devs):
    b = pltpu.get_barrier_semaphore()
    for d in devs:
        pl.semaphore_signal(b, inc=1, device_id=d, device_id_type=MESH)
    pl.semaphore_wait(b, len(devs))


def run(*gens):
    live = []
    for g in gens:
        t = next(g, None)
        if t is not None:
            live.append([t, g])
    while live:
        e = min(live, key=lambda v: v[0])
        t = next(e[1], None)
        if t is None:
            live.remove(e)
        else:
            e[0] = t


def ring_ag(cm, own, blk, half, m, plus, minus, t0, u):
    lo, hi = (m + 3) % 4, (m + 1) % 4
    p0 = cm.send(own, blk(m), plus)
    m0 = cm.send(own, blk(m), minus)
    yield t0 + u
    p0.wait_recv()
    p1 = cm.send(half(lo, 0), half(lo, 0), plus)
    m0.wait_recv()
    m1 = cm.send(half(hi, 1), half(hi, 1), minus)
    yield t0 + 1.5 * u
    p1.wait_recv()
    m1.wait_recv()


def k1(x, g, wg, wu, n_o, wg_o, wu_o, xs_o, g_o, xs, gb, nb, wst, ssem, rsem, lsem):
    p = Pos()
    cm = Comm(ssem, rsem, lsem)
    barrier([p.H(d) for d in range(1, 8)] + [p.Y(1), p.Y(-1), p.Z(1), p.Z(-1)])
    tb = xs.shape[1]
    ww = wst.shape[2]

    def rows(q):
        return x.at[pl.ds(pl.multiple_of(1024 * q + tb * p.f, tb), tb), :]

    xin = []
    for d in range(1, 8):
        t = p.H(d)
        xin.append(cm.send(rows(quarter(t[1])), xs.at[p.h], t))
        xin.append(cm.send(g, gb.at[p.h], t))
    loc = [cm.local(rows(p.q), xs.at[p.h]), cm.local(g, gb.at[p.h])]

    def cols(w, j):
        return w.at[:, pl.ds(pl.multiple_of(ww * j, ww), ww)]

    def weights():
        ws = ((wg, wg_o), (wu, wu_o))
        stage = [cm.local(cols(w, p.j), wst.at[k]) for k, (w, _) in enumerate(ws)]
        b, a, c = [], [], []
        for w, wo in ws:
            b.append(cm.send(cols(w, 1 - p.j), wo.at[p.h], p.B))
            a.append(cm.send(cols(w, p.j), wo.at[p.h], p.A))
            c.append(cm.send(cols(w, p.j), wo.at[p.h], p.C))
        yield 8.0
        out = []
        for k, (w, wo) in enumerate(ws):
            stage[k].wait()
            out.append(cm.local(wst.at[k], wo.at[p.h]))
        a2 = []
        for k, (w, wo) in enumerate(ws):
            yield 14.0 + 12.5 * k
            b[k].wait_recv()
            s = wo.at[p.B[1]]
            a2.append(cm.send(s, s, p.A))
            c.append(cm.send(s, s, p.C))
            a[k].wait_recv()
            s = wo.at[p.A[1]]
            c.append(cm.send(s, s, p.C))
        for k, (w, wo) in enumerate(ws):
            yield 40.0 + 12.5 * k
            a2[k].wait_recv()
            s = wo.at[(2 * (3 - p.A[1] // 2)) + p.c]
            c.append(cm.send(s, s, p.C))
        yield 55.0
        for v in c:
            v.wait_recv()
        for v in out:
            v.wait()

    def tokens():
        yield 5.0
        for v in xin:
            v.wait_recv()
        for v in loc:
            v.wait()
        ss = jnp.zeros((tb, 1), F32)
        for k in range(8):
            v = xs[k].astype(F32)
            ss = ss + jnp.sum(v * v, axis=-1, keepdims=True)
        r = lax.rsqrt(ss / 3072.0 + EPS)
        dh = xs.shape[2]
        for k in range(8):
            nb[:, dh * k:dh * (k + 1)] = (xs[k].astype(F32) * r * gb[k, 0:1, :]).astype(BF)
        xs_o[...] = xs[...]
        g_o[...] = gb[...]
        yield from plane_ag(cm, p, nb, n_o, 10.0, 4.0, 17.0)

    run(tokens(), weights())
    cm.finish()


def plane_ag(cm, p, nb, n_o, t0, u1, u2):
    hb = nb.shape[0] // 2
    w = nb.shape[1] // 2
    ca, cb = pl.ds(0, w), pl.ds(w, w)
    own = cm.local(nb, n_o.at[p.z, p.y])

    def first():
        ya = ring_ag(cm, nb.at[:, ca], lambda i: n_o.at[p.z, i, :, ca],
                     lambda i, s: n_o.at[p.z, i, pl.ds(hb * s, hb), ca], p.y, p.Y(1), p.Y(-1), t0, u1)
        zb = ring_ag(cm, nb.at[:, cb], lambda i: n_o.at[i, p.y, :, cb],
                     lambda i, s: n_o.at[i, p.y, pl.ds(hb * s, hb), cb], p.z, p.Z(1), p.Z(-1), t0, u1)
        for t, _ in zip(ya, zb):
            yield t
        list(zb)

    yield from first()
    own.wait()
    t1 = t0 + 1.5 * u1

    def second():
        za = ring_ag(cm, n_o.at[p.z, :, :, ca], lambda i: n_o.at[i, :, :, ca],
                     lambda i, s: n_o.at[i, pl.ds(2 * s, 2), :, ca], p.z, p.Z(1), p.Z(-1), t1, u2)
        yb = ring_ag(cm, n_o.at[:, p.y, :, cb], lambda i: n_o.at[:, i, :, cb],
                     lambda i, s: n_o.at[pl.ds(2 * s, 2), i, :, cb], p.y, p.Y(1), p.Y(-1), t1, u2)
        for t, _ in zip(za, yb):
            yield t
        list(yb)

    yield from second()


def k2(a, wd, wo, a_o, wd_o, wo_o, dst, ost, ssem, rsem, lsem):
    p = Pos()
    cm = Comm(ssem, rsem, lsem)
    barrier([p.A, p.B, p.C])
    w = wd.shape[1]

    def slot(o, h):
        return o.at[:, pl.ds(pl.multiple_of(w * (h % 4), w), w)]

    ra = cm.send(a, a_o, p.B)
    st = [cm.local(wd, dst), cm.local(wo, ost)]
    fa = [cm.send(wd, slot(wd_o, p.h), p.A), cm.send(wo, slot(wo_o, p.h), p.A)]
    c = [cm.send(wd, slot(wd_o, p.h), p.C), cm.send(wo, slot(wo_o, p.h), p.C)]
    out = []
    for v, s, o in zip(st, (dst, ost), (wd_o, wo_o)):
        v.wait()
        out.append(cm.local(s, slot(o, p.h)))
    for v, o in zip(fa, (wd_o, wo_o)):
        v.wait_recv()
        s = slot(o, p.A[1])
        c.append(cm.send(s, s, p.C))
    for v in c:
        v.wait_recv()
    for v in out:
        v.wait()
    ra.wait_recv()
    cm.finish()


def ring_rs(cm, get, r1p, r1m, ap, am, fp, fm, res, m, plus, minus, t0, u):
    lo, hi, far = (m + 3) % 4, (m + 1) % 4, (m + 2) % 4
    hb = r1p.shape[-2]
    f0, f1 = (Ellipsis, pl.ds(0, hb), slice(None)), (Ellipsis, pl.ds(hb, hb), slice(None))
    p0 = cm.send(get(far, 0), r1p, plus)
    m0 = cm.send(get(far, 1), r1m, minus)
    p1 = cm.send(get(hi, 1), fp.at[f1], plus)
    m1 = cm.send(get(lo, 0), fm.at[f0], minus)
    yield t0 + 0.5 * u
    p0.wait_recv()
    ap[...] = r1p[...] + get(hi, 0)[...]
    p2 = cm.send(ap, fp.at[f0], plus)
    m0.wait_recv()
    am[...] = r1m[...] + get(lo, 1)[...]
    m2 = cm.send(am, fm.at[f1], minus)
    yield t0 + u
    p1.wait_recv()
    m1.wait_recv()
    yield t0 + 1.5 * u
    p2.wait_recv()
    m2.wait_recv()
    res[f0] = (fp[f0] + fm[f0]) + get(m, 0)[...]
    res[f1] = (fp[f1] + fm[f1]) + get(m, 1)[...]


def k3(y, xs, g, wq, xn_o, n_o, wq_o,
       r1, a1, f1, s1, r2, a2, f2, s2, xr, nbuf, wst, ssem, rsem, lsem):
    p = Pos()
    cm = Comm(ssem, rsem, lsem)
    barrier([p.Y(1), p.Y(-1), p.Z(1), p.Z(-1), p.H(2), p.H(-2), p.B, p.C])
    tb = y.shape[2]
    hb = tb // 2
    w = y.shape[3] // 2
    ca, cb = pl.ds(0, w), pl.ds(w, w)

    def weights():
        st = cm.local(wq, wst)
        c = [cm.send(wq, wq_o.at[p.h], p.C)]

        def blk(i):
            return wq_o.at[2 * i + p.c]

        hr = wq.shape[0] // 2

        def half(i, s):
            return wq_o.at[2 * i + p.c, pl.ds(hr * s, hr), :]

        m = p.x
        lo, hi, far = (m + 3) % 4, (m + 1) % 4, (m + 2) % 4
        p0 = cm.send(wq, blk(m), p.H(2))
        m0 = cm.send(wq, blk(m), p.H(-2))
        yield 1.0
        st.wait()
        own = cm.local(wst, wq_o.at[p.h])
        yield 16.0
        p0.wait_recv()
        p1 = cm.send(half(lo, 0), half(lo, 0), p.H(2))
        c.append(cm.send(blk(lo), blk(lo), p.C))
        m0.wait_recv()
        m1 = cm.send(half(hi, 1), half(hi, 1), p.H(-2))
        c.append(cm.send(blk(hi), blk(hi), p.C))
        yield 28.0
        p1.wait_recv()
        m1.wait_recv()
        c.append(cm.send(blk(far), blk(far), p.C))
        yield 34.0
        own.wait()
        for v in c:
            v.wait_recv()

    def tokens():
        ga = ring_rs(cm, lambda i, s: y.at[:, i, pl.ds(hb * s, hb), ca], r1.at[0], r1.at[1], a1.at[0], a1.at[1],
                     f1.at[0], f1.at[1], s1.at[0], p.y, p.Y(1), p.Y(-1), 0.0, 17.0)
        gb = ring_rs(cm, lambda i, s: y.at[i, :, pl.ds(hb * s, hb), cb], r1.at[2], r1.at[3], a1.at[2], a1.at[3],
                     f1.at[2], f1.at[3], s1.at[1], p.z, p.Z(1), p.Z(-1), 0.0, 17.0)
        for t, _ in zip(ga, gb):
            yield t
        list(gb)
        ga = ring_rs(cm, lambda i, s: s1.at[0, i, pl.ds(hb * s, hb), :], r2.at[0], r2.at[1], a2.at[0], a2.at[1],
                     f2.at[0], f2.at[1], s2.at[0], p.z, p.Z(1), p.Z(-1), 26.0, 6.0)
        gb = ring_rs(cm, lambda i, s: s1.at[1, i, pl.ds(hb * s, hb), :], r2.at[2], r2.at[3], a2.at[2], a2.at[3],
                     f2.at[2], f2.at[3], s2.at[1], p.y, p.Y(1), p.Y(-1), 26.0, 6.0)
        for t, _ in zip(ga, gb):
            yield t
        list(gb)
        dh = xs.shape[2]
        for k in range(4):
            yk = s2[k // 2, :, dh * (k % 2):dh * (k % 2 + 1)]
            xn_o[:, dh * k:dh * (k + 1)] = (xs[4 * p.j + k].astype(F32) + yk).astype(BF)
        ex = cm.send(xn_o.at[pl.ds(pl.multiple_of(hb * (1 - p.j), hb), hb), :], xr, p.B)
        mine = xn_o[pl.ds(pl.multiple_of(hb * p.j, hb), hb), :].astype(F32)
        ss = jnp.sum(mine * mine, axis=-1, keepdims=True)
        yield 36.0
        ex.wait_recv()
        oth = xr[...].astype(F32)
        ss = ss + jnp.sum(oth * oth, axis=-1, keepdims=True)
        r = lax.rsqrt(ss / 3072.0 + EPS)
        for k in range(4):
            cs = slice(dh * k, dh * (k + 1))
            nbuf[p.j, :, cs] = (mine[:, cs] * r * g[4 * p.j + k, 1:2, :]).astype(BF)
            nbuf[1 - p.j, :, cs] = (oth[:, cs] * r * g[4 * (1 - p.j) + k, 1:2, :]).astype(BF)
        yield from plane_ag2(cm, p, nbuf, n_o, 38.0, 2.0, 8.5)

    run(tokens(), weights())
    cm.finish()


def plane_ag2(cm, p, nb, n_o, t0, u1, u2):
    hb = nb.shape[1] // 2
    w = nb.shape[2]
    ca, cb = pl.ds(0, w), pl.ds(w, w)
    own = [cm.local(nb.at[0], n_o.at[p.z, p.y, :, ca]), cm.local(nb.at[1], n_o.at[p.z, p.y, :, cb])]
    ya = ring_ag(cm, nb.at[0], lambda i: n_o.at[p.z, i, :, ca],
                 lambda i, s: n_o.at[p.z, i, pl.ds(hb * s, hb), ca], p.y, p.Y(1), p.Y(-1), t0, u1)
    zb = ring_ag(cm, nb.at[1], lambda i: n_o.at[i, p.y, :, cb],
                 lambda i, s: n_o.at[i, p.y, pl.ds(hb * s, hb), cb], p.z, p.Z(1), p.Z(-1), t0, u1)
    for t, _ in zip(ya, zb):
        yield t
    list(zb)
    for v in own:
        v.wait()
    t1 = t0 + 1.5 * u1
    za = ring_ag(cm, n_o.at[p.z, :, :, ca], lambda i: n_o.at[i, :, :, ca],
                 lambda i, s: n_o.at[i, pl.ds(2 * s, 2), :, ca], p.z, p.Z(1), p.Z(-1), t1, u2)
    yb = ring_ag(cm, n_o.at[:, p.y, :, cb], lambda i: n_o.at[:, i, :, cb],
                 lambda i, s: n_o.at[pl.ds(2 * s, 2), i, :, cb], p.y, p.Y(1), p.Y(-1), t1, u2)
    for t, _ in zip(za, yb):
        yield t
    list(yb)


def k5(qkv, xn, q_o, x_o, xq, ssem, rsem, lsem):
    p = Pos()
    cm = Comm(ssem, rsem, lsem)
    barrier([p.Y(1), p.Y(-1), p.Z(1), p.Z(-1), p.H(2), p.H(-2), p.A, p.C, p.AC])
    dh = xq.shape[2]

    def cols(h):
        return xn.at[:, pl.ds(pl.multiple_of(dh * (h % 4), dh), dh)]

    ex = [cm.send(cols(d[1]), xq.at[p.q], d) for d in (p.A, p.C, p.AC)]
    lo = cm.local(cols(p.h), xq.at[p.q])

    def proj():
        def blk(x, c):
            h = 2 * x + c
            return q_o.at[quarter(h), :, h // 4]

        def half(x, c, s):
            h = 2 * x + c
            return q_o.at[quarter(h), pl.ds(8 * s, 8), h // 4]

        m = p.x
        l, r, far = (m + 3) % 4, (m + 1) % 4, (m + 2) % 4
        own = cm.local(qkv, blk(m, p.c))
        p0 = cm.send(qkv, blk(m, p.c), p.H(2))
        m0 = cm.send(qkv, blk(m, p.c), p.H(-2))
        c = [cm.send(qkv, blk(m, p.c), p.C)]
        yield 17.5
        p0.wait_recv()
        s = half(l, p.c, 0)
        p1 = cm.send(s, s, p.H(2))
        m0.wait_recv()
        s = half(r, p.c, 1)
        m1 = cm.send(s, s, p.H(-2))
        for b in (blk(l, p.c), blk(r, p.c)):
            c.append(cm.send(b, b, p.C))
        yield 28.0
        p1.wait_recv()
        s = half(far, p.c, 0)
        c.append(cm.send(s, s, p.C))
        m1.wait_recv()
        s = half(far, p.c, 1)
        c.append(cm.send(s, s, p.C))
        own.wait()
        for v in c:
            v.wait_recv()

    def resid():
        yield 3.0
        for v in ex:
            v.wait_recv()
        lo.wait()
        qa, qb = pl.ds(0, 2), pl.ds(2, 2)
        own = cm.local(xq, x_o.at[:, p.z, p.y])
        ya = ring_ag(cm, xq.at[qa], lambda i: x_o.at[qa, p.z, i],
                     lambda i, s: x_o.at[s, p.z, i], p.y, p.Y(1), p.Y(-1), 3.5, 2.0)
        zb = ring_ag(cm, xq.at[qb], lambda i: x_o.at[qb, i, p.y],
                     lambda i, s: x_o.at[2 + s, i, p.y], p.z, p.Z(1), p.Z(-1), 3.5, 2.0)
        for t, _ in zip(ya, zb):
            yield t
        list(zb)
        own.wait()
        za = ring_ag(cm, x_o.at[qa, p.z], lambda i: x_o.at[qa, i],
                     lambda i, s: x_o.at[s, i], p.z, p.Z(1), p.Z(-1), 7.0, 8.5)
        yb = ring_ag(cm, x_o.at[qb, :, p.y], lambda i: x_o.at[qb, :, i],
                     lambda i, s: x_o.at[2 + s, :, i], p.y, p.Y(1), p.Y(-1), 7.0, 8.5)
        for t, _ in zip(za, yb):
            yield t
        list(yb)

    run(resid(), proj())
    cm.finish()


def _call(body, cid, out, out_specs, in_specs, scratch, args, nsem=64, nl=8):
    return pl.pallas_call(
        body,
        out_shape=[jax.ShapeDtypeStruct(s, d) for s, d in out],
        in_specs=in_specs,
        out_specs=out_specs,
        scratch_shapes=scratch + [pltpu.SemaphoreType.DMA((nsem,)), pltpu.SemaphoreType.DMA((nsem,)),
                                  pltpu.SemaphoreType.DMA((nl,))],
        compiler_params=pltpu.CompilerParams(collective_id=cid, has_side_effects=True,
                                             vmem_limit_bytes=48 * 1024 * 1024),
        name=body.__name__,
    )(*args)


def solution(mesh):
    def body(x, g1, g2, w_gate, w_up, w_down, o, w_o, w_qkv):
        t, dh = x.shape
        d = dh * 8
        ff = w_gate.shape[1]
        tq = t // 4
        tb = tq // 16
        h = lax.axis_index('h')
        q = quarter(h)
        j = h // 4
        g = jnp.concatenate([jnp.stack([g1, g2]), jnp.zeros((6, dh), F32)], axis=0)
        fh = ff // 2
        n, wg, wu, xs, gf = _call(
            k1, 1,
            [((4, 4, tb, d), BF), ((8, dh, fh), BF), ((8, dh, fh), BF), ((8, tb, dh), BF), ((8, 8, dh), F32)],
            [ANY, ANY, ANY, VM, VM], [ANY] * 4,
            [pltpu.VMEM((8, tb, dh), BF), pltpu.VMEM((8, 8, dh), F32), pltpu.VMEM((tb, d), BF),
             pltpu.VMEM((2, dh, fh), BF)],
            (x, g, w_gate, w_up))
        n = n.reshape(tq, d)
        gt = _dot(n, wg.reshape(d, fh))
        up = _dot(n, wu.reshape(d, fh))
        a = (jax.nn.silu(gt) * up).astype(BF)
        a2, wd, wo = _call(
            k2, 2, [((tq, fh), BF), ((ff, d // 2), BF), ((w_o.shape[0], d // 2), BF)],
            [ANY] * 3, [ANY] * 3,
            [pltpu.VMEM(w_down.shape, BF), pltpu.VMEM(w_o.shape, BF)],
            (a, w_down, w_o))
        ot = lax.dynamic_slice(o, (q * tq, 0), (tq, o.shape[1]))
        wd0 = lax.dynamic_slice(wd, (j * fh, 0), (fh, d // 2))
        wd1 = lax.dynamic_slice(wd, ((1 - j) * fh, 0), (fh, d // 2))
        y = _dot(a, wd0) + _dot(a2, wd1) + _dot(ot, wo)
        w2 = d // 4
        hb = tb // 2
        xn, n1, wq = _call(
            k3, 3,
            [((tb, d // 2), BF), ((4, 4, hb, d), BF), ((8, dh, w_qkv.shape[1]), BF)],
            [VM, ANY, ANY], [VM, VM, VM, ANY],
            [pltpu.VMEM((4, 4, hb, w2), F32), pltpu.VMEM((4, 4, hb, w2), F32), pltpu.VMEM((4, 4, tb, w2), F32),
             pltpu.VMEM((2, 4, tb, w2), F32),
             pltpu.VMEM((4, hb, w2), F32), pltpu.VMEM((4, hb, w2), F32), pltpu.VMEM((4, tb, w2), F32),
             pltpu.VMEM((2, tb, w2), F32),
             pltpu.VMEM((hb, d // 2), BF), pltpu.VMEM((2, hb, d // 2), BF), pltpu.VMEM(w_qkv.shape, BF)],
            (y.reshape(4, 4, tb, d // 2), xs, gf, w_qkv))
        qkv = _dot(n1.reshape(tq // 2, d), wq.reshape(d, -1)).astype(BF)
        qo, xo = _call(
            k5, 4,
            [((4, 16, 2, hb, qkv.shape[1]), BF), ((4, 4, 4, tb, dh), BF)],
            [ANY, ANY], [VM, VM],
            [pltpu.VMEM((4, tb, dh), BF)],
            (qkv.reshape(16, hb, -1), xn))
        return xo.reshape(t, dh), qo.reshape(t, -1)

    in_specs = (P(None, 'h'), P('h'), P('h'), P('h', 'f'), P('h', 'f'), P('f', 'h'),
                P(None, 'f'), P('f', 'h'), P('h', 'f'))
    return jax.shard_map(body, mesh=mesh, in_specs=in_specs,
                         out_specs=(P(None, 'h'), P(None, 'f')), check_vma=False)
```

```python
import functools

import jax
import jax.numpy as jnp
from jax import lax
from jax.experimental import pallas as pl
from jax.experimental.pallas import tpu as pltpu
from jax.sharding import PartitionSpec as P

EPS = 1e-6
MESH = pl.DeviceIdType.MESH
ANY = pl.BlockSpec(memory_space=pl.ANY)
VM = pl.BlockSpec(memory_space=pltpu.VMEM)
HB = pl.BlockSpec(memory_space=pltpu.HBM)
BF = jnp.bfloat16
F32 = jnp.float32


def _dot(a, b):
    return jnp.dot(a, b, preferred_element_type=jnp.float32)


class Pos:
    def __init__(self):
        self.f = lax.axis_index('f')
        self.h = lax.axis_index('h')
        self.z, self.y = self.f // 4, self.f % 4
        self.x, self.c = self.h // 2, self.h % 2
        self.j = self.x // 2
        self.q = quarter(self.h)
        ax = self.x + 1 - 2 * (self.x % 2)
        self.A = (self.f, 2 * ax + self.c)
        self.B = (self.f, 2 * (3 - self.x) + self.c)
        self.C = (self.f, self.h + 1 - 2 * self.c)
        self.AC = (self.f, 2 * ax + 1 - self.c)

    def H(self, d):
        return (self.f, (self.h + d) % 8)

    def Y(self, d):
        return (4 * self.z + (self.y + d) % 4, self.h)

    def Z(self, d):
        return (4 * ((self.z + d) % 4) + self.y, self.h)


def quarter(h):
    x = h // 2
    return 2 * ((x + x // 2) % 2) + h % 2


class Comm:
    def __init__(self, ssem, rsem, lsem):
        self.ssem, self.rsem, self.lsem = ssem, rsem, lsem
        self.k = 0
        self.lk = 0
        self.sent = []

    def send(self, src, dst, dev):
        c = pltpu.make_async_remote_copy(src_ref=src, dst_ref=dst, send_sem=self.ssem.at[self.k],
                                         recv_sem=self.rsem.at[self.k], device_id=dev, device_id_type=MESH)
        self.k += 1
        c.start()
        self.sent.append(c)
        return c

    def local(self, src, dst):
        c = pltpu.make_async_copy(src, dst, self.lsem.at[self.lk])
        self.lk += 1
        c.start()
        return c

    def finish(self):
        for c in self.sent:
            c.wait_send()


def barrier(devs):
    b = pltpu.get_barrier_semaphore()
    for d in devs:
        pl.semaphore_signal(b, inc=1, device_id=d, device_id_type=MESH)
    pl.semaphore_wait(b, len(devs))


def run(*gens):
    live = []
    for g in gens:
        t = next(g, None)
        if t is not None:
            live.append([t, g])
    while live:
        e = min(live, key=lambda v: v[0])
        t = next(e[1], None)
        if t is None:
            live.remove(e)
        else:
            e[0] = t


def ring_ag(cm, own, blk, half, m, plus, minus, t0, u):
    lo, hi = (m + 3) % 4, (m + 1) % 4
    p0 = cm.send(own, blk(m), plus)
    m0 = cm.send(own, blk(m), minus)
    yield t0 + u
    p0.wait_recv()
    p1 = cm.send(half(lo, 0), half(lo, 0), plus)
    m0.wait_recv()
    m1 = cm.send(half(hi, 1), half(hi, 1), minus)
    yield t0 + 1.5 * u
    p1.wait_recv()
    m1.wait_recv()


def mlp(x, g, wg, wu, wd, o, wo, y_o, xs_o, g_o,
        xs, gb, nb, n, wgb, wub, wdb, wob, ov, a1, a2, ssem, rsem, lsem):
    p = Pos()
    cm = Comm(ssem, rsem, lsem)
    barrier([p.H(d) for d in range(1, 8)] + [p.Y(1), p.Y(-1), p.Z(1), p.Z(-1)])
    tb, dh = xs.shape[1:]
    ww = wgb.shape[2]
    hb = tb // 2

    def rows(q):
        return x.at[pl.ds(pl.multiple_of(1024 * q + tb * p.f, tb), tb), :]

    xin = []
    for d in range(1, 8):
        t = p.H(d)
        xin.append(cm.send(rows(quarter(t[1])), xs.at[p.h], t))
        xin.append(cm.send(g, gb.at[p.h], t))
    loc = [cm.local(rows(p.q), xs.at[p.h]), cm.local(g, gb.at[p.h])]

    def cols(w, j):
        return w.at[:, pl.ds(pl.multiple_of(ww * j, ww), ww)]

    def slot(b, h):
        return b.at[:, pl.ds(pl.multiple_of(dh * (h % 4), dh), dh)]

    late = []
    down_in = []

    def weights():
        ws = ((wg, wgb), (wu, wub))
        own, b, a, c, a2_ = [], [], [], [], []
        for w, wb in ws:
            b.append(cm.send(cols(w, 1 - p.j), wb.at[p.h], p.B))
            a.append(cm.send(cols(w, p.j), wb.at[p.h], p.A))
            c.append(cm.send(cols(w, p.j), wb.at[p.h], p.C))
            own.append(cm.local(cols(w, p.j), wb.at[p.h]))
        own.append(cm.local(o.at[pl.ds(pl.multiple_of(1024 * p.q, 1024), 1024), :], ov))
        for w, wb in ((wd, wdb), (wo, wob)):
            own.append(cm.local(w, slot(wb, p.h)))
        for k, (w, wb) in enumerate(ws):
            yield 14.0 + 12.5 * k
            b[k].wait_recv()
            s = wb.at[p.B[1]]
            a2_.append(cm.send(s, s, p.A))
            c.append(cm.send(s, s, p.C))
            a[k].wait_recv()
            s = wb.at[p.A[1]]
            c.append(cm.send(s, s, p.C))
        for w, wb in ((wd, wdb), (wo, wob)):
            down_in.append(cm.send(w, slot(wb, p.h), p.A))
            late.append(cm.send(w, slot(wb, p.h), p.C))
        for k, (w, wb) in enumerate(ws):
            yield 40.0 + 12.5 * k
            a2_[k].wait_recv()
            s = wb.at[(2 * (3 - p.A[1] // 2)) + p.c]
            c.append(cm.send(s, s, p.C))
        yield 55.0
        for v in c:
            v.wait_recv()
        for v in own:
            v.wait()

    def tokens():
        yield 5.0
        for v in xin:
            v.wait_recv()
        for v in loc:
            v.wait()
        ss = jnp.zeros((tb, 1), F32)
        for k in range(8):
            v = xs[k].astype(F32)
            ss = ss + jnp.sum(v * v, axis=-1, keepdims=True)
        r = lax.rsqrt(ss / 3072.0 + EPS)
        for k in range(8):
            nb[:, dh * k:dh * (k + 1)] = (xs[k].astype(F32) * r * gb[k, 0:1, :]).astype(BF)
        xs_o[...] = xs[...]
        g_o[...] = gb[...]
        yield from plane_ag(cm, p, nb, n, 10.0, 4.0, 17.0)

    run(tokens(), weights())

    tn = 256
    d = n.shape[3]
    got = []
    for b in range(4):
        s, zh = b // 2, b % 2

        def gate_up(t, carry, b=b, s=s, zh=zh):
            v = n[2 * zh:2 * zh + 2, :, hb * s:hb * (s + 1), :].reshape(8 * hb, d)
            cs = pl.ds(pl.multiple_of(t * tn, tn), tn)
            gt = _dot(v, wgb[:, :, cs].reshape(d, tn))
            up = _dot(v, wub[:, :, cs].reshape(d, tn))
            a1[b, :, cs] = (jax.nn.silu(gt) * up).astype(BF)
            return carry

        lax.fori_loop(0, ww // tn, gate_up, 0)
        got.append(cm.send(a1.at[b], a2.at[b], p.B))

    for v, wb in zip(down_in, (wdb, wob)):
        v.wait_recv()
        s = slot(wb, p.A[1])
        late.append(cm.send(s, s, p.C))
    for v in late:
        v.wait_recv()
    kn = 512
    for b in range(4):
        s, zh = b // 2, b % 2
        got[b].wait_recv()

        def down(t, carry, b=b, s=s, zh=zh):
            cs = pl.ds(pl.multiple_of(t * kn, kn), kn)
            ob = ov[512 * zh:512 * (zh + 1), :].reshape(8, tb, -1)[:, hb * s:hb * (s + 1), :].reshape(8 * hb, -1)
            v = (_dot(a1[b], wdb[pl.ds(pl.multiple_of(ww * p.j, ww), ww), cs])
                 + _dot(a2[b], wdb[pl.ds(pl.multiple_of(ww * (1 - p.j), ww), ww), cs])
                 + _dot(ob, wob[:, cs]))
            y_o[2 * zh:2 * zh + 2, :, hb * s:hb * (s + 1), cs] = v.reshape(2, 4, hb, kn)
            return carry

        lax.fori_loop(0, wdb.shape[1] // kn, down, 0)
    cm.finish()


def plane_ag(cm, p, nb, n_o, t0, u1, u2):
    hb = nb.shape[0] // 2
    w = nb.shape[1] // 2
    ca, cb = pl.ds(0, w), pl.ds(w, w)
    own = cm.local(nb, n_o.at[p.z, p.y])

    def first():
        ya = ring_ag(cm, nb.at[:, ca], lambda i: n_o.at[p.z, i, :, ca],
                     lambda i, s: n_o.at[p.z, i, pl.ds(hb * s, hb), ca], p.y, p.Y(1), p.Y(-1), t0, u1)
        zb = ring_ag(cm, nb.at[:, cb], lambda i: n_o.at[i, p.y, :, cb],
                     lambda i, s: n_o.at[i, p.y, pl.ds(hb * s, hb), cb], p.z, p.Z(1), p.Z(-1), t0, u1)
        for t, _ in zip(ya, zb):
            yield t
        list(zb)

    yield from first()
    own.wait()
    t1 = t0 + 1.5 * u1

    def second():
        za = ring_ag(cm, n_o.at[p.z, :, :, ca], lambda i: n_o.at[i, :, :, ca],
                     lambda i, s: n_o.at[i, pl.ds(2 * s, 2), :, ca], p.z, p.Z(1), p.Z(-1), t1, u2)
        yb = ring_ag(cm, n_o.at[:, p.y, :, cb], lambda i: n_o.at[:, i, :, cb],
                     lambda i, s: n_o.at[pl.ds(2 * s, 2), i, :, cb], p.y, p.Y(1), p.Y(-1), t1, u2)
        for t, _ in zip(za, yb):
            yield t
        list(yb)

    yield from second()


def ring_rs(cm, get, r1p, r1m, ap, am, fp, fm, res, m, plus, minus, t0, u):
    lo, hi, far = (m + 3) % 4, (m + 1) % 4, (m + 2) % 4
    hb = r1p.shape[-2]
    f0, f1 = (Ellipsis, pl.ds(0, hb), slice(None)), (Ellipsis, pl.ds(hb, hb), slice(None))
    p0 = cm.send(get(far, 0), r1p, plus)
    m0 = cm.send(get(far, 1), r1m, minus)
    p1 = cm.send(get(hi, 1), fp.at[f1], plus)
    m1 = cm.send(get(lo, 0), fm.at[f0], minus)
    yield t0 + 0.5 * u
    p0.wait_recv()
    ap[...] = r1p[...] + get(hi, 0)[...]
    p2 = cm.send(ap, fp.at[f0], plus)
    m0.wait_recv()
    am[...] = r1m[...] + get(lo, 1)[...]
    m2 = cm.send(am, fm.at[f1], minus)
    yield t0 + u
    p1.wait_recv()
    m1.wait_recv()
    yield t0 + 1.5 * u
    p2.wait_recv()
    m2.wait_recv()
    res[f0] = (fp[f0] + fm[f0]) + get(m, 0)[...]
    res[f1] = (fp[f1] + fm[f1]) + get(m, 1)[...]


def k3(y, xs, g, wq, xn_o, n_o, wq_o,
       r1, a1, f1, s1, r2, a2, f2, s2, xr, nbuf, wst, ssem, rsem, lsem):
    p = Pos()
    cm = Comm(ssem, rsem, lsem)
    barrier([p.Y(1), p.Y(-1), p.Z(1), p.Z(-1), p.H(2), p.H(-2), p.B, p.C])
    tb = y.shape[2]
    hb = tb // 2
    w = y.shape[3] // 2
    ca, cb = pl.ds(0, w), pl.ds(w, w)

    def weights():
        st = cm.local(wq, wst)
        c = [cm.send(wq, wq_o.at[p.h], p.C)]

        def blk(i):
            return wq_o.at[2 * i + p.c]

        hr = wq.shape[0] // 2

        def half(i, s):
            return wq_o.at[2 * i + p.c, pl.ds(hr * s, hr), :]

        m = p.x
        lo, hi, far = (m + 3) % 4, (m + 1) % 4, (m + 2) % 4
        p0 = cm.send(wq, blk(m), p.H(2))
        m0 = cm.send(wq, blk(m), p.H(-2))
        yield 1.0
        st.wait()
        own = cm.local(wst, wq_o.at[p.h])
        yield 16.0
        p0.wait_recv()
        p1 = cm.send(half(lo, 0), half(lo, 0), p.H(2))
        c.append(cm.send(blk(lo), blk(lo), p.C))
        m0.wait_recv()
        m1 = cm.send(half(hi, 1), half(hi, 1), p.H(-2))
        c.append(cm.send(blk(hi), blk(hi), p.C))
        yield 28.0
        p1.wait_recv()
        m1.wait_recv()
        c.append(cm.send(blk(far), blk(far), p.C))
        yield 34.0
        own.wait()
        for v in c:
            v.wait_recv()

    def tokens():
        ga = ring_rs(cm, lambda i, s: y.at[:, i, pl.ds(hb * s, hb), ca], r1.at[0], r1.at[1], a1.at[0], a1.at[1],
                     f1.at[0], f1.at[1], s1.at[0], p.y, p.Y(1), p.Y(-1), 0.0, 17.0)
        gb = ring_rs(cm, lambda i, s: y.at[i, :, pl.ds(hb * s, hb), cb], r1.at[2], r1.at[3], a1.at[2], a1.at[3],
                     f1.at[2], f1.at[3], s1.at[1], p.z, p.Z(1), p.Z(-1), 0.0, 17.0)
        for t, _ in zip(ga, gb):
            yield t
        list(gb)
        ga = ring_rs(cm, lambda i, s: s1.at[0, i, pl.ds(hb * s, hb), :], r2.at[0], r2.at[1], a2.at[0], a2.at[1],
                     f2.at[0], f2.at[1], s2.at[0], p.z, p.Z(1), p.Z(-1), 26.0, 6.0)
        gb = ring_rs(cm, lambda i, s: s1.at[1, i, pl.ds(hb * s, hb), :], r2.at[2], r2.at[3], a2.at[2], a2.at[3],
                     f2.at[2], f2.at[3], s2.at[1], p.y, p.Y(1), p.Y(-1), 26.0, 6.0)
        for t, _ in zip(ga, gb):
            yield t
        list(gb)
        dh = xs.shape[2]
        for k in range(4):
            yk = s2[k // 2, :, dh * (k % 2):dh * (k % 2 + 1)]
            xn_o[:, dh * k:dh * (k + 1)] = (xs[4 * p.j + k].astype(F32) + yk).astype(BF)
        ex = cm.send(xn_o.at[pl.ds(pl.multiple_of(hb * (1 - p.j), hb), hb), :], xr, p.B)
        mine = xn_o[pl.ds(pl.multiple_of(hb * p.j, hb), hb), :].astype(F32)
        ss = jnp.sum(mine * mine, axis=-1, keepdims=True)
        yield 36.0
        ex.wait_recv()
        oth = xr[...].astype(F32)
        ss = ss + jnp.sum(oth * oth, axis=-1, keepdims=True)
        r = lax.rsqrt(ss / 3072.0 + EPS)
        for k in range(4):
            cs = slice(dh * k, dh * (k + 1))
            nbuf[p.j, :, cs] = (mine[:, cs] * r * g[4 * p.j + k, 1:2, :]).astype(BF)
            nbuf[1 - p.j, :, cs] = (oth[:, cs] * r * g[4 * (1 - p.j) + k, 1:2, :]).astype(BF)
        yield from plane_ag2(cm, p, nbuf, n_o, 38.0, 2.0, 8.5)

    run(tokens(), weights())
    cm.finish()


def plane_ag2(cm, p, nb, n_o, t0, u1, u2):
    hb = nb.shape[1] // 2
    w = nb.shape[2]
    ca, cb = pl.ds(0, w), pl.ds(w, w)
    own = [cm.local(nb.at[0], n_o.at[p.z, p.y, :, ca]), cm.local(nb.at[1], n_o.at[p.z, p.y, :, cb])]
    ya = ring_ag(cm, nb.at[0], lambda i: n_o.at[p.z, i, :, ca],
                 lambda i, s: n_o.at[p.z, i, pl.ds(hb * s, hb), ca], p.y, p.Y(1), p.Y(-1), t0, u1)
    zb = ring_ag(cm, nb.at[1], lambda i: n_o.at[i, p.y, :, cb],
                 lambda i, s: n_o.at[i, p.y, pl.ds(hb * s, hb), cb], p.z, p.Z(1), p.Z(-1), t0, u1)
    for t, _ in zip(ya, zb):
        yield t
    list(zb)
    for v in own:
        v.wait()
    t1 = t0 + 1.5 * u1
    za = ring_ag(cm, n_o.at[p.z, :, :, ca], lambda i: n_o.at[i, :, :, ca],
                 lambda i, s: n_o.at[i, pl.ds(2 * s, 2), :, ca], p.z, p.Z(1), p.Z(-1), t1, u2)
    yb = ring_ag(cm, n_o.at[:, p.y, :, cb], lambda i: n_o.at[:, i, :, cb],
                 lambda i, s: n_o.at[pl.ds(2 * s, 2), i, :, cb], p.y, p.Y(1), p.Y(-1), t1, u2)
    for t, _ in zip(za, yb):
        yield t
    list(yb)


def k5(qkv, xn, q_o, x_o, xq, ssem, rsem, lsem):
    p = Pos()
    cm = Comm(ssem, rsem, lsem)
    barrier([p.Y(1), p.Y(-1), p.Z(1), p.Z(-1), p.H(2), p.H(-2), p.A, p.C, p.AC])
    dh = xq.shape[2]

    def cols(h):
        return xn.at[:, pl.ds(pl.multiple_of(dh * (h % 4), dh), dh)]

    ex = [cm.send(cols(d[1]), xq.at[p.q], d) for d in (p.A, p.C, p.AC)]
    lo = cm.local(cols(p.h), xq.at[p.q])

    def proj():
        def blk(x, c):
            h = 2 * x + c
            return q_o.at[quarter(h), :, h // 4]

        def half(x, c, s):
            h = 2 * x + c
            return q_o.at[quarter(h), pl.ds(8 * s, 8), h // 4]

        m = p.x
        l, r, far = (m + 3) % 4, (m + 1) % 4, (m + 2) % 4
        own = cm.local(qkv, blk(m, p.c))
        p0 = cm.send(qkv, blk(m, p.c), p.H(2))
        m0 = cm.send(qkv, blk(m, p.c), p.H(-2))
        c = [cm.send(qkv, blk(m, p.c), p.C)]
        yield 17.5
        p0.wait_recv()
        s = half(l, p.c, 0)
        p1 = cm.send(s, s, p.H(2))
        m0.wait_recv()
        s = half(r, p.c, 1)
        m1 = cm.send(s, s, p.H(-2))
        for b in (blk(l, p.c), blk(r, p.c)):
            c.append(cm.send(b, b, p.C))
        yield 28.0
        p1.wait_recv()
        s = half(far, p.c, 0)
        c.append(cm.send(s, s, p.C))
        m1.wait_recv()
        s = half(far, p.c, 1)
        c.append(cm.send(s, s, p.C))
        own.wait()
        for v in c:
            v.wait_recv()

    def resid():
        yield 3.0
        for v in ex:
            v.wait_recv()
        lo.wait()
        qa, qb = pl.ds(0, 2), pl.ds(2, 2)
        own = cm.local(xq, x_o.at[:, p.z, p.y])
        ya = ring_ag(cm, xq.at[qa], lambda i: x_o.at[qa, p.z, i],
                     lambda i, s: x_o.at[s, p.z, i], p.y, p.Y(1), p.Y(-1), 3.5, 2.0)
        zb = ring_ag(cm, xq.at[qb], lambda i: x_o.at[qb, i, p.y],
                     lambda i, s: x_o.at[2 + s, i, p.y], p.z, p.Z(1), p.Z(-1), 3.5, 2.0)
        for t, _ in zip(ya, zb):
            yield t
        list(zb)
        own.wait()
        za = ring_ag(cm, x_o.at[qa, p.z], lambda i: x_o.at[qa, i],
                     lambda i, s: x_o.at[s, i], p.z, p.Z(1), p.Z(-1), 7.0, 8.5)
        yb = ring_ag(cm, x_o.at[qb, :, p.y], lambda i: x_o.at[qb, :, i],
                     lambda i, s: x_o.at[2 + s, :, i], p.y, p.Y(1), p.Y(-1), 7.0, 8.5)
        for t, _ in zip(za, yb):
            yield t
        list(yb)

    run(resid(), proj())
    cm.finish()


def _call(body, cid, out, out_specs, in_specs, scratch, args, nsem=64, nl=12):
    return pl.pallas_call(
        body,
        out_shape=[jax.ShapeDtypeStruct(s, d) for s, d in out],
        in_specs=in_specs,
        out_specs=out_specs,
        scratch_shapes=scratch + [pltpu.SemaphoreType.DMA((nsem,)), pltpu.SemaphoreType.DMA((nsem,)),
                                  pltpu.SemaphoreType.DMA((nl,))],
        compiler_params=pltpu.CompilerParams(collective_id=cid, has_side_effects=True,
                                             vmem_limit_bytes=56 * 1024 * 1024),
        name=body.__name__,
    )(*args)


def solution(mesh):
    def body(x, g1, g2, w_gate, w_up, w_down, o, w_o, w_qkv):
        t, dh = x.shape
        d = dh * 8
        ff = w_gate.shape[1]
        tq = t // 4
        tb = tq // 16
        g = jnp.concatenate([jnp.stack([g1, g2]), jnp.zeros((6, dh), F32)], axis=0)
        fh = ff // 2
        bf, f32 = (lambda *v: pltpu.VMEM(v, BF)), (lambda *v: pltpu.VMEM(v, F32))
        y, xs, gf = _call(
            mlp, 1,
            [((4, 4, tb, d // 2), F32), ((8, tb, dh), BF), ((8, 8, dh), F32)],
            [VM, VM, VM], [HB] * 7,
            [bf(8, tb, dh), f32(8, 8, dh), bf(tb, d), bf(4, 4, tb, d), bf(8, dh, fh), bf(8, dh, fh),
             bf(ff, d // 2), bf(w_o.shape[0], d // 2), bf(tq, w_o.shape[0]), bf(4, tq // 4, fh), bf(4, tq // 4, fh)],
            (x, g, w_gate, w_up, w_down, o, w_o))
        w2 = d // 4
        hb = tb // 2
        xn, n1, wq = _call(
            k3, 3,
            [((tb, d // 2), BF), ((4, 4, hb, d), BF), ((8, dh, w_qkv.shape[1]), BF)],
            [VM, ANY, ANY], [VM, VM, VM, HB],
            [pltpu.VMEM((4, 4, hb, w2), F32), pltpu.VMEM((4, 4, hb, w2), F32), pltpu.VMEM((4, 4, tb, w2), F32),
             pltpu.VMEM((2, 4, tb, w2), F32),
             pltpu.VMEM((4, hb, w2), F32), pltpu.VMEM((4, hb, w2), F32), pltpu.VMEM((4, tb, w2), F32),
             pltpu.VMEM((2, tb, w2), F32),
             pltpu.VMEM((hb, d // 2), BF), pltpu.VMEM((2, hb, d // 2), BF), pltpu.VMEM(w_qkv.shape, BF)],
            (y, xs, gf, w_qkv))
        qkv = _dot(n1.reshape(tq // 2, d), wq.reshape(d, -1)).astype(BF)
        qo, xo = _call(
            k5, 4,
            [((4, 16, 2, hb, qkv.shape[1]), BF), ((4, 4, 4, tb, dh), BF)],
            [ANY, ANY], [VM, VM],
            [pltpu.VMEM((4, tb, dh), BF)],
            (qkv.reshape(16, hb, -1), xn))
        return xo.reshape(t, dh), qo.reshape(t, -1)

    in_specs = (P(None, 'h'), P('h'), P('h'), P('h', 'f'), P('h', 'f'), P('f', 'h'),
                P(None, 'f'), P('f', 'h'), P('h', 'f'))
    return jax.shard_map(body, mesh=mesh, in_specs=in_specs,
                         out_specs=(P(None, 'h'), P(None, 'f')), check_vma=False)
```

```python
import functools

import jax
import jax.numpy as jnp
from jax import lax
from jax.experimental import pallas as pl
from jax.experimental.pallas import tpu as pltpu
from jax.sharding import PartitionSpec as P

EPS = 1e-6
MESH = pl.DeviceIdType.MESH
ANY = pl.BlockSpec(memory_space=pl.ANY)
VM = pl.BlockSpec(memory_space=pltpu.VMEM)
HB = pl.BlockSpec(memory_space=pltpu.HBM)
BF = jnp.bfloat16
F32 = jnp.float32


def _dot(a, b):
    return jnp.dot(a, b, preferred_element_type=jnp.float32)


class Pos:
    def __init__(self):
        self.f = lax.axis_index('f')
        self.h = lax.axis_index('h')
        self.z, self.y = self.f // 4, self.f % 4
        self.x, self.c = self.h // 2, self.h % 2
        self.j = self.x // 2
        self.q = quarter(self.h)
        ax = self.x + 1 - 2 * (self.x % 2)
        self.A = (self.f, 2 * ax + self.c)
        self.B = (self.f, 2 * (3 - self.x) + self.c)
        self.C = (self.f, self.h + 1 - 2 * self.c)
        self.AC = (self.f, 2 * ax + 1 - self.c)

    def H(self, d):
        return (self.f, (self.h + d) % 8)

    def Y(self, d):
        return (4 * self.z + (self.y + d) % 4, self.h)

    def Z(self, d):
        return (4 * ((self.z + d) % 4) + self.y, self.h)


def quarter(h):
    x = h // 2
    return 2 * ((x + x // 2) % 2) + h % 2


class Comm:
    def __init__(self, ssem, rsem, lsem):
        self.ssem, self.rsem, self.lsem = ssem, rsem, lsem
        self.k = 0
        self.lk = 0
        self.sent = []

    def send(self, src, dst, dev):
        c = pltpu.make_async_remote_copy(src_ref=src, dst_ref=dst, send_sem=self.ssem.at[self.k],
                                         recv_sem=self.rsem.at[self.k], device_id=dev, device_id_type=MESH)
        self.k += 1
        c.start()
        self.sent.append(c)
        return c

    def local(self, src, dst):
        c = pltpu.make_async_copy(src, dst, self.lsem.at[self.lk])
        self.lk += 1
        c.start()
        return c

    def finish(self):
        for c in self.sent:
            c.wait_send()


def barrier(devs):
    b = pltpu.get_barrier_semaphore()
    for d in devs:
        pl.semaphore_signal(b, inc=1, device_id=d, device_id_type=MESH)
    pl.semaphore_wait(b, len(devs))


def run(*gens):
    live = []
    for g in gens:
        t = next(g, None)
        if t is not None:
            live.append([t, g])
    while live:
        e = min(live, key=lambda v: v[0])
        t = next(e[1], None)
        if t is None:
            live.remove(e)
        else:
            e[0] = t


def ring_ag(cm, own, blk, half, m, plus, minus, t0, u):
    lo, hi = (m + 3) % 4, (m + 1) % 4
    p0 = cm.send(own, blk(m), plus)
    m0 = cm.send(own, blk(m), minus)
    yield t0 + u
    p0.wait_recv()
    p1 = cm.send(half(lo, 0), half(lo, 0), plus)
    m0.wait_recv()
    m1 = cm.send(half(hi, 1), half(hi, 1), minus)
    yield t0 + 1.5 * u
    p1.wait_recv()
    m1.wait_recv()


def plane_ag(cm, p, own, n_o, half, t0, u1, u2):
    ya = ring_ag(cm, own(0), lambda i: n_o(p.z, i, 0), lambda i, s: half(n_o(p.z, i, 0), s), p.y, p.Y(1), p.Y(-1), t0, u1)
    zb = ring_ag(cm, own(1), lambda i: n_o(i, p.y, 1), lambda i, s: half(n_o(i, p.y, 1), s), p.z, p.Z(1), p.Z(-1), t0, u1)
    loc = [cm.local(own(k), n_o(p.z, p.y, k)) for k in range(2)]
    for t, _ in zip(ya, zb):
        yield t
    list(zb)
    for v in loc:
        v.wait()
    t1 = t0 + 1.5 * u1 + 2.0
    al, h2 = slice(None), lambda s: pl.ds(2 * s, 2)
    za = ring_ag(cm, n_o(p.z, al, 0), lambda i: n_o(i, al, 0), lambda i, s: n_o(i, h2(s), 0), p.z, p.Z(1), p.Z(-1), t1, u2)
    yb = ring_ag(cm, n_o(al, p.y, 1), lambda i: n_o(al, i, 1), lambda i, s: n_o(h2(s), i, 1), p.y, p.Y(1), p.Y(-1), t1, u2)
    for t, _ in zip(za, yb):
        yield t
    list(yb)


def ring_rs(cm, get, r1p, r1m, ap, am, fp, fm, res, m, plus, minus, t0, u):
    lo, hi, far = (m + 3) % 4, (m + 1) % 4, (m + 2) % 4
    hb = r1p.shape[-2]
    f0, f1 = (Ellipsis, pl.ds(0, hb), slice(None)), (Ellipsis, pl.ds(hb, hb), slice(None))
    p0 = cm.send(get(far, 0), r1p, plus)
    m0 = cm.send(get(far, 1), r1m, minus)
    p1 = cm.send(get(hi, 1), fp.at[f1], plus)
    m1 = cm.send(get(lo, 0), fm.at[f0], minus)
    yield t0 + 0.5 * u
    p0.wait_recv()
    ap[...] = r1p[...] + get(hi, 0)[...]
    p2 = cm.send(ap, fp.at[f0], plus)
    m0.wait_recv()
    am[...] = r1m[...] + get(lo, 1)[...]
    m2 = cm.send(am, fm.at[f1], minus)
    yield t0 + u
    p1.wait_recv()
    m1.wait_recv()
    yield t0 + 1.5 * u
    p2.wait_recv()
    m2.wait_recv()
    res[f0] = (fp[f0] + fm[f0]) + get(m, 0)[...]
    res[f1] = (fp[f1] + fm[f1]) + get(m, 1)[...]


def block(x, g, wg, wu, wd, o, wo, wq, x_o, q_o,
          xs, gb, nb, n, wgb, wub, wdb, wob, wqb, ov, a1, a2, y,
          r1, c1, f1, s1, r2, c2, f2, s2, xn, xr, nh, n1, qk, xq, ssem, rsem, lsem):
    p = Pos()
    cm = Comm(ssem, rsem, lsem)
    barrier([p.H(d) for d in range(1, 8)] + [p.Y(1), p.Y(-1), p.Z(1), p.Z(-1)])
    tb, dh = xs.shape[1:]
    ww = wgb.shape[2]
    d = n.shape[3]
    dc = d // 2
    hb = tb // 2
    qb = hb // 2
    al = slice(None)

    def dyn(i, m):
        return pl.ds(pl.multiple_of(i * m, m), m)

    def rows(q):
        return x.at[pl.ds(pl.multiple_of(1024 * q + tb * p.f, tb), tb), :]

    xin = []
    for k in range(1, 8):
        t = p.H(k)
        xin.append(cm.send(rows(quarter(t[1])), xs.at[p.h], t))
        xin.append(cm.send(g, gb.at[p.h], t))
    loc = [cm.local(rows(p.q), xs.at[p.h]), cm.local(g, gb.at[p.h])]

    def cols(w, j):
        return w.at[:, dyn(j, ww)]

    def slot(b, h):
        return b.at[:, dyn(h % 4, dh)]

    down_in, late, got = [], [], []

    def weights():
        ws = ((wg, wgb), (wu, wub))
        own, b, a, c, a2_ = [], [], [], [], []
        for w, wb in ws:
            b.append(cm.send(cols(w, 1 - p.j), wb.at[p.h], p.B))
            a.append(cm.send(cols(w, p.j), wb.at[p.h], p.A))
            c.append(cm.send(cols(w, p.j), wb.at[p.h], p.C))
            own.append(cm.local(cols(w, p.j), wb.at[p.h]))
        own.append(cm.local(o.at[pl.ds(pl.multiple_of(1024 * p.q, 1024), 1024), :], ov))
        for w, wb in ((wd, wdb), (wo, wob)):
            own.append(cm.local(w, slot(wb, p.h)))
        own.append(cm.local(wq, wqb.at[p.h]))
        for k, (w, wb) in enumerate(ws):
            yield 17.0 + 12.5 * k
            b[k].wait_recv()
            s = wb.at[p.B[1]]
            a2_.append(cm.send(s, s, p.A))
            c.append(cm.send(s, s, p.C))
            a[k].wait_recv()
            s = wb.at[p.A[1]]
            c.append(cm.send(s, s, p.C))
        for w, wb in ((wd, wdb), (wo, wob)):
            down_in.append(cm.send(w, slot(wb, p.h), p.A))
            late.append(cm.send(w, slot(wb, p.h), p.C))
        for k, (w, wb) in enumerate(ws):
            yield 46.0 + 12.5 * k
            a2_[k].wait_recv()
            s = wb.at[(2 * (3 - p.A[1] // 2)) + p.c]
            c.append(cm.send(s, s, p.C))
        yield 60.0
        for v in c:
            v.wait_recv()
        for v in own:
            v.wait()

    def tokens():
        yield 5.0
        for v in xin:
            v.wait_recv()
        for v in loc:
            v.wait()
        ss = jnp.zeros((tb, 1), F32)
        for k in range(8):
            v = xs[k].astype(F32)
            ss = ss + jnp.sum(v * v, axis=-1, keepdims=True)
        r = lax.rsqrt(ss / float(d) + EPS)
        for k in range(8):
            nb[:, dh * k:dh * (k + 1)] = (xs[k].astype(F32) * r * gb[k, 0:1, :]).astype(BF)
        part = (pl.ds(0, dc), pl.ds(dc, dc))
        yield from plane_ag(cm, p, lambda k: nb.at[:, part[k]], lambda zi, yi, k: n.at[zi, yi, :, part[k]],
                            lambda v, s: v.at[pl.ds(hb * s, hb), :], 13.0, 6.0, 17.0)

    run(tokens(), weights())

    tn = 256
    for b in range(4):
        s, zh = b // 2, b % 2

        def gate_up(t, carry, b=b, s=s, zh=zh):
            v = n[2 * zh:2 * zh + 2, :, hb * s:hb * (s + 1), :].reshape(8 * hb, d)
            cs = dyn(t, tn)
            gt = _dot(v, wgb[:, :, cs].reshape(d, tn))
            up = _dot(v, wub[:, :, cs].reshape(d, tn))
            a1[b, :, cs] = (jax.nn.silu(gt) * up).astype(BF)
            return carry

        lax.fori_loop(0, ww // tn, gate_up, 0)
        got.append(cm.send(a1.at[b], a2.at[b], p.B))

    qc = []
    m = p.x
    lo, hi, far = (m + 3) % 4, (m + 1) % 4, (m + 2) % 4

    def qweights():
        def blk(i):
            return wqb.at[2 * i + p.c]

        hr = wq.shape[0] // 2

        def half(i, s):
            return wqb.at[2 * i + p.c, pl.ds(hr * s, hr), :]

        p0 = cm.send(wq, blk(m), p.H(2))
        m0 = cm.send(wq, blk(m), p.H(-2))
        qc.append(cm.send(wq, blk(m), p.C))
        yield 112.0
        p0.wait_recv()
        p1 = cm.send(half(lo, 0), half(lo, 0), p.H(2))
        qc.append(cm.send(blk(lo), blk(lo), p.C))
        m0.wait_recv()
        m1 = cm.send(half(hi, 1), half(hi, 1), p.H(-2))
        qc.append(cm.send(blk(hi), blk(hi), p.C))
        yield 120.0
        p1.wait_recv()
        m1.wait_recv()
        qc.append(cm.send(blk(far), blk(far), p.C))
        yield 127.0
        for v in qc:
            v.wait_recv()

    kn = 512

    def down(b):
        s, zh = b // 2, b % 2
        got[b].wait_recv()

        def step(t, carry):
            cs = dyn(t, kn)
            ob = ov[512 * zh:512 * (zh + 1), :].reshape(8, tb, -1)[:, hb * s:hb * (s + 1), :].reshape(8 * hb, -1)
            v = (_dot(a1[b], wdb[dyn(p.j, ww), cs]) + _dot(a2[b], wdb[dyn(1 - p.j, ww), cs]) + _dot(ob, wob[:, cs]))
            y[s, 2 * zh:2 * zh + 2, :, :, cs] = v.reshape(2, 4, hb, kn)
            return carry

        lax.fori_loop(0, wdb.shape[1] // kn, step, 0)

    xex = []

    def chain(s, t0):
        if s == 0:
            yield 84.0
            for v, wb in zip(down_in, (wdb, wob)):
                v.wait_recv()
                sl = slot(wb, p.A[1])
                late.append(cm.send(sl, sl, p.C))
            yield 87.0
            for v in late:
                v.wait_recv()
        else:
            yield t0 - 8.0
        down(2 * s)
        yield t0 - 2.0
        down(2 * s + 1)
        ca, cb = pl.ds(0, dc // 2), pl.ds(dc // 2, dc // 2)

        def both(get_a, get_b, r, c, f, res, ax_a, ax_b, t, u):
            ga = ring_rs(cm, get_a, r.at[s, 0], r.at[s, 1], c.at[s, 0], c.at[s, 1], f.at[s, 0], f.at[s, 1],
                         res.at[s, 0], *ax_a, t, u)
            gb_ = ring_rs(cm, get_b, r.at[s, 2], r.at[s, 3], c.at[s, 2], c.at[s, 3], f.at[s, 2], f.at[s, 3],
                          res.at[s, 1], *ax_b, t, u)
            for v, _ in zip(ga, gb_):
                yield v
            list(gb_)

        ay, az = (p.y, p.Y(1), p.Y(-1)), (p.z, p.Z(1), p.Z(-1))
        yield from both(lambda i, k: y.at[s, :, i, pl.ds(qb * k, qb), ca], lambda i, k: y.at[s, i, :, pl.ds(qb * k, qb), cb],
                        r1, c1, f1, s1, ay, az, t0 + 1.5, 8.5)
        yield from both(lambda i, k: s1.at[s, 0, i, pl.ds(qb * k, qb), :], lambda i, k: s1.at[s, 1, i, pl.ds(qb * k, qb), :],
                        r2, c2, f2, s2, az, ay, t0 + 14.5, 3.0)
        t = t0 + 20.0
        rs = pl.ds(hb * s, hb)
        for k in range(4):
            yk = s2[s, k // 2, :, dh * (k % 2):dh * (k % 2 + 1)]
            xn[s, :, dh * k:dh * (k + 1)] = (xs[4 * p.j + k, rs, :].astype(F32) + yk).astype(BF)
        ex = cm.send(xn.at[s, dyn(1 - p.j, qb), :], xr.at[s], p.B)
        for v in (p.A, p.C, p.AC):
            xex.append(cm.send(xn.at[s, :, dyn(v[1] % 4, dh)], xq.at[p.q, rs, :], v).wait_recv)
        xex.append(cm.local(xn.at[s, :, dyn(p.h % 4, dh)], xq.at[p.q, rs, :]).wait)
        mine = xn[s, dyn(p.j, qb), :].astype(F32)
        yield t + 2.0
        ex.wait_recv()
        oth = xr[s].astype(F32)
        ss = jnp.sum(mine * mine, axis=-1, keepdims=True) + jnp.sum(oth * oth, axis=-1, keepdims=True)
        r = lax.rsqrt(ss / float(d) + EPS)
        for k in range(4):
            cs = slice(dh * k, dh * (k + 1))
            nh[s, p.j, :, cs] = (mine[:, cs] * r * gb[4 * p.j + k, 1:2, :]).astype(BF)
            nh[s, 1 - p.j, :, cs] = (oth[:, cs] * r * gb[4 * (1 - p.j) + k, 1:2, :]).astype(BF)
        part = (pl.ds(0, dc), pl.ds(dc, dc))
        hd = dc // 2
        yield from plane_ag(cm, p, lambda k: nh.at[s, k], lambda zi, yi, k: n1.at[s, zi, yi, :, part[k]],
                            lambda v, k: v.at[:, pl.ds(hd * k, hd)], t + 3.0, 2.5, 6.0)
        yield t + 20.0

        if s == 0:
            for _ in qw:
                pass

        def proj(t_, carry):
            cs = dyn(t_, tn)
            qk[s, :, :, cs] = _dot(n1[s].reshape(16 * qb, d), wqb[:, :, cs].reshape(d, tn)).astype(BF).reshape(16, qb, tn)
            return carry

        lax.fori_loop(0, wq.shape[1] // tn, proj, 0)

        def blk(xx):
            h = 2 * xx + p.c
            return q_o.at[quarter(h), :, s, h // 4]

        def half(xx, k):
            h = 2 * xx + p.c
            return q_o.at[quarter(h), pl.ds(8 * k, 8), s, h // 4]

        own = cm.local(qk.at[s], blk(m))
        p0 = cm.send(qk.at[s], blk(m), p.H(2))
        m0 = cm.send(qk.at[s], blk(m), p.H(-2))
        c = [cm.send(qk.at[s], blk(m), p.C)]
        yield t + 31.0
        p0.wait_recv()
        p1 = cm.send(half(lo, 0), half(lo, 0), p.H(2))
        m0.wait_recv()
        m1 = cm.send(half(hi, 1), half(hi, 1), p.H(-2))
        for b in (blk(lo), blk(hi)):
            c.append(cm.send(b, b, p.C))
        yield t + 38.0
        p1.wait_recv()
        c.append(cm.send(half(far, 0), half(far, 0), p.C))
        m1.wait_recv()
        c.append(cm.send(half(far, 1), half(far, 1), p.C))
        yield t + 42.0
        own.wait()
        for v in c:
            v.wait_recv()

    def resid():
        yield 134.0
        for wait in xex:
            wait()
        yield from plane_ag(cm, p, lambda k: xq.at[pl.ds(2 * k, 2)], lambda zi, yi, k: x_o.at[pl.ds(2 * k, 2), zi, yi],
                            lambda v, k: v.at[k], 138.0, 3.0, 10.0)

    def qrest():
        yield next(qw)
        yield from qw

    qw = qweights()
    run(qrest(), chain(0, 91.0), chain(1, 103.0), resid())
    cm.finish()


def solution(mesh):
    def body(x, g1, g2, w_gate, w_up, w_down, o, w_o, w_qkv):
        t, dh = x.shape
        d = dh * 8
        ff = w_gate.shape[1]
        tq = t // 4
        tb = tq // 16
        fh = ff // 2
        hb, qb, w2, nq = tb // 2, tb // 4, d // 4, w_qkv.shape[1]
        g = jnp.concatenate([jnp.stack([g1, g2]), jnp.zeros((6, dh), F32)], axis=0)
        bf, f32 = (lambda *v: pltpu.VMEM(v, BF)), (lambda *v: pltpu.VMEM(v, F32))
        ns = 208
        xo, qo = pl.pallas_call(
            block,
            out_shape=[jax.ShapeDtypeStruct((4, 4, 4, tb, dh), BF), jax.ShapeDtypeStruct((4, 16, 2, 2, qb, nq), BF)],
            in_specs=[HB] * 8,
            out_specs=[ANY] * 2,
            scratch_shapes=[
                bf(8, tb, dh), f32(8, 8, dh), bf(tb, d), bf(4, 4, tb, d), bf(8, dh, fh), bf(8, dh, fh),
                bf(ff, d // 2), bf(w_o.shape[0], d // 2), bf(8, dh, nq), bf(tq, w_o.shape[0]),
                bf(4, tq // 4, fh), bf(4, tq // 4, fh), f32(2, 4, 4, hb, d // 2),
                f32(2, 4, 4, qb, w2), f32(2, 4, 4, qb, w2), f32(2, 4, 4, hb, w2), f32(2, 2, 4, hb, w2),
                f32(2, 4, qb, w2), f32(2, 4, qb, w2), f32(2, 4, hb, w2), f32(2, 2, hb, w2),
                bf(2, hb, d // 2), bf(2, qb, d // 2), bf(2, 2, qb, d // 2), bf(2, 4, 4, qb, d), bf(2, 16, qb, nq),
                bf(4, tb, dh),
                pltpu.SemaphoreType.DMA((ns,)), pltpu.SemaphoreType.DMA((ns,)), pltpu.SemaphoreType.DMA((28,))],
            compiler_params=pltpu.CompilerParams(collective_id=1, has_side_effects=True,
                                                 vmem_limit_bytes=63 * 1024 * 1024),
            name='block',
        )(x, g, w_gate, w_up, w_down, o, w_o, w_qkv)
        return xo.reshape(t, dh), qo.reshape(t, -1)

    in_specs = (P(None, 'h'), P('h'), P('h'), P('h', 'f'), P('h', 'f'), P('f', 'h'),
                P(None, 'f'), P('f', 'h'), P('h', 'f'))
    return jax.shard_map(body, mesh=mesh, in_specs=in_specs,
                         out_specs=(P(None, 'h'), P(None, 'f')), check_vma=False)
```

```python
import functools

import jax
import jax.numpy as jnp
from jax import lax
from jax.experimental import pallas as pl
from jax.experimental.pallas import tpu as pltpu
from jax.sharding import PartitionSpec as P

EPS = 1e-6
VLIM = 56 * 1024 * 1024
MESH = pl.DeviceIdType.MESH
ANY = pl.BlockSpec(memory_space=pl.ANY)
VM = pl.BlockSpec(memory_space=pltpu.VMEM)
HB = pl.BlockSpec(memory_space=pltpu.HBM)
BF = jnp.bfloat16
F32 = jnp.float32


def _dot(a, b):
    return jnp.dot(a, b, preferred_element_type=jnp.float32)


class Pos:
    def __init__(self):
        self.f = lax.axis_index('f')
        self.h = lax.axis_index('h')
        self.z, self.y = self.f // 4, self.f % 4
        self.x, self.c = self.h // 2, self.h % 2
        self.j = self.x // 2
        self.q = quarter(self.h)
        ax = self.x + 1 - 2 * (self.x % 2)
        self.A = (self.f, 2 * ax + self.c)
        self.B = (self.f, 2 * (3 - self.x) + self.c)
        self.C = (self.f, self.h + 1 - 2 * self.c)
        self.AC = (self.f, 2 * ax + 1 - self.c)

    def H(self, d):
        return (self.f, (self.h + d) % 8)

    def Y(self, d):
        return (4 * self.z + (self.y + d) % 4, self.h)

    def Z(self, d):
        return (4 * ((self.z + d) % 4) + self.y, self.h)


def quarter(h):
    x = h // 2
    return 2 * ((x + x // 2) % 2) + h % 2


class Comm:
    def __init__(self, ssem, rsem, lsem):
        self.ssem, self.rsem, self.lsem = ssem, rsem, lsem
        self.k = 0
        self.lk = 0
        self.sent = []

    def send(self, src, dst, dev):
        c = pltpu.make_async_remote_copy(src_ref=src, dst_ref=dst, send_sem=self.ssem.at[self.k],
                                         recv_sem=self.rsem.at[self.k], device_id=dev, device_id_type=MESH)
        self.k += 1
        c.start()
        self.sent.append(c)
        return c

    def local(self, src, dst):
        c = pltpu.make_async_copy(src, dst, self.lsem.at[self.lk])
        self.lk += 1
        c.start()
        return c

    def finish(self):
        for c in self.sent:
            c.wait_send()


class Part(Comm):
    def __init__(self, cm):
        self.cm = cm
        self.sent = []

    def send(self, src, dst, dev):
        c = self.cm.send(src, dst, dev)
        self.sent.append(self.cm.sent.pop())
        return c

    def local(self, src, dst):
        return self.cm.local(src, dst)


def barrier(devs):
    b = pltpu.get_barrier_semaphore()
    for d in devs:
        pl.semaphore_signal(b, inc=1, device_id=d, device_id_type=MESH)
    pl.semaphore_wait(b, len(devs))


def run(*gens):
    live = []
    for g in gens:
        t = next(g, None)
        if t is not None:
            live.append([t, g])
    while live:
        e = min(live, key=lambda v: v[0])
        t = next(e[1], None)
        if t is None:
            live.remove(e)
        else:
            e[0] = t


def ring_ag(cm, own, blk, half, m, plus, minus, t0, u):
    lo, hi = (m + 3) % 4, (m + 1) % 4
    p0 = cm.send(own, blk(m), plus)
    m0 = cm.send(own, blk(m), minus)
    yield t0 + u
    p0.wait_recv()
    p1 = cm.send(half(lo, 0), half(lo, 0), plus)
    m0.wait_recv()
    m1 = cm.send(half(hi, 1), half(hi, 1), minus)
    yield t0 + 1.5 * u
    p1.wait_recv()
    m1.wait_recv()


def ring_direct(cm, own, blk, m, sides, t0, u):
    c = [cm.send(own, blk(m), v) for v in sides]
    yield t0 + u
    for v in c:
        v.wait_recv()


def plane_ag(cm, p, own, n_o, half, t0, u1, u2):
    if half is None:
        ya = ring_direct(cm, own(0), lambda i: n_o(p.z, i, 0), p.y, (p.Y(1), p.Y(-1), p.Y(2)), t0, u1)
        zb = ring_direct(cm, own(1), lambda i: n_o(i, p.y, 1), p.z, (p.Z(1), p.Z(-1), p.Z(2)), t0, u1)
    else:
        ya = ring_ag(cm, own(0), lambda i: n_o(p.z, i, 0), lambda i, s: half(n_o(p.z, i, 0), s), p.y, p.Y(1), p.Y(-1), t0, u1)
        zb = ring_ag(cm, own(1), lambda i: n_o(i, p.y, 1), lambda i, s: half(n_o(i, p.y, 1), s), p.z, p.Z(1), p.Z(-1), t0, u1)
    loc = [cm.local(own(k), n_o(p.z, p.y, k)) for k in range(2)]
    for t, _ in zip(ya, zb):
        yield t
    list(zb)
    for v in loc:
        v.wait()
    t1 = t0 + (u1 if half is None else 1.5 * u1 + 2.0)
    al, h2 = slice(None), lambda s: pl.ds(2 * s, 2)
    za = ring_ag(cm, n_o(p.z, al, 0), lambda i: n_o(i, al, 0), lambda i, s: n_o(i, h2(s), 0), p.z, p.Z(1), p.Z(-1), t1, u2)
    yb = ring_ag(cm, n_o(al, p.y, 1), lambda i: n_o(al, i, 1), lambda i, s: n_o(h2(s), i, 1), p.y, p.Y(1), p.Y(-1), t1, u2)
    for t, _ in zip(za, yb):
        yield t
    list(yb)


def ring_rs(cm, get, r1p, r1m, fp, fm, res, m, plus, minus, t0, u):
    lo, hi, far = (m + 3) % 4, (m + 1) % 4, (m + 2) % 4
    hb = r1p.shape[-2]
    f0, f1 = (Ellipsis, pl.ds(0, hb), slice(None)), (Ellipsis, pl.ds(hb, hb), slice(None))
    p0 = cm.send(get(far, 0), r1p, plus)
    m0 = cm.send(get(far, 1), r1m, minus)
    p1 = cm.send(get(hi, 1), fp.at[f1], plus)
    m1 = cm.send(get(lo, 0), fm.at[f0], minus)
    yield t0 + 0.5 * u
    p0.wait_recv()
    v = get(hi, 0)
    v[...] = r1p[...] + v[...]
    p2 = cm.send(v, fp.at[f0], plus)
    m0.wait_recv()
    v = get(lo, 1)
    v[...] = r1m[...] + v[...]
    m2 = cm.send(v, fm.at[f1], minus)
    yield t0 + u
    p1.wait_recv()
    m1.wait_recv()
    yield t0 + 1.5 * u
    p2.wait_recv()
    m2.wait_recv()
    res(0)[...] = (fp[f0] + fm[f0]) + get(m, 0)[...]
    res(1)[...] = (fp[f1] + fm[f1]) + get(m, 1)[...]


def block(x, g, wg, wu, wd, o, wo, wq, x_o, q_o,
          xs, gb, nb, n, wgb, wub, wdb, wob, wqb, ov, a1, a2, y,
          r1, f1, r2, f2, s2, xn, xr, nh, qk, xq, ssem, rsem, lsem):
    p = Pos()
    cm = Comm(ssem, rsem, lsem)
    barrier([p.H(k) for k in range(1, 8)] + [p.Y(k) for k in range(1, 4)] + [p.Z(k) for k in range(1, 4)])
    tb, dh = xs.shape[1:]
    ww = wgb.shape[2]
    d = n.shape[3]
    dc = d // 2
    hb = tb // 2
    qb = hb // 2
    al = slice(None)

    def dyn(i, m):
        return pl.ds(pl.multiple_of(i * m, m), m)

    def rows(q):
        return x.at[pl.ds(pl.multiple_of(1024 * q + tb * p.f, tb), tb), :]

    xin = []
    for k in range(1, 8):
        t = p.H(k)
        xin.append(cm.send(rows(quarter(t[1])), xs.at[p.h], t))
        xin.append(cm.send(g, gb.at[p.h], t))
    loc = [cm.local(rows(p.q), xs.at[p.h]), cm.local(g, gb.at[p.h])]

    cw = ((0, 512), (512, 256))

    def cols(w, j, k):
        return w.at[:, pl.ds(pl.multiple_of(ww * j + cw[k][0], 128), cw[k][1])]

    def part_of(b, h, k):
        return b.at[h, :, pl.ds(*cw[k])]

    def slot(b, h):
        return b.at[:, dyn(h % 4, dh)]

    down_in, late, got, own = [], [], [[], []], []
    cn = Part(cm)
    ready = [[], []]

    def weights():
        ws = ((wg, wgb), (wu, wub))
        fb, fa, f2_ = [[], []], [[], []], [[], []]
        opp = 2 * (3 - p.A[1] // 2) + p.c

        def fan(k, to_b, to_a):
            for w, wb in ws:
                dst = part_of(wb, p.h, k)
                if to_b:
                    fb[k].append(cm.send(cols(w, 1 - p.j, k), dst, p.B))
                if to_a:
                    fa[k].append(cm.send(cols(w, p.j, k), dst, p.A))
                    ready[k].append(cm.send(cols(w, p.j, k), dst, p.C).wait_recv)
                    ready[k].append(cm.local(cols(w, p.j, k), dst).wait)

        def take(c, wb, h, k, onward):
            c.wait_recv()
            v = part_of(wb, h, k)
            if onward:
                f2_[k].append(cm.send(v, v, p.A))
            ready[k].append(cm.send(v, v, p.C).wait_recv)

        fan(0, True, True)
        fan(1, True, False)
        own.append(cm.local(o.at[pl.ds(pl.multiple_of(1024 * p.q, 1024), 1024), :], ov))
        for w, wb in ((wd, wdb), (wo, wob)):
            own.append(cm.local(w, slot(wb, p.h)))
        own.append(cm.local(wq, wqb.at[p.h]))
        for k in range(2):
            yield 14.0 + 8.0 * k
            take(fb[0][k], ws[k][1], p.B[1], 0, True)
            take(fa[0][k], ws[k][1], p.A[1], 0, False)
        fan(1, False, True)
        yield 31.0
        for k in range(2):
            take(fb[1][k], ws[k][1], p.B[1], 1, True)
        hk = wd.shape[0] // 2
        down_in.append((cm.send(wo, slot(wob, p.h), p.A), slot(wob, p.A[1])))
        late.append(cm.send(wo, slot(wob, p.h), p.C))
        for r in range(2):
            down_in.append((cm.send(wd.at[pl.ds(hk * r, hk), :], slot(wdb, p.h).at[pl.ds(hk * r, hk), :], p.A),
                            slot(wdb, p.A[1]).at[pl.ds(hk * r, hk), :]))
        late.append(cm.send(wd, slot(wdb, p.h), p.C))
        for k in range(2):
            yield 34.0 + 7.0 * k
            take(f2_[0][k], ws[k][1], opp, 0, False)
        yield 49.0
        for k in range(2):
            take(fa[1][k], ws[k][1], p.A[1], 1, False)
        for k in range(2):
            yield 56.0 + 4.5 * k
            take(f2_[1][k], ws[k][1], opp, 1, False)

    def tokens():
        yield 5.0
        for v in xin:
            v.wait_recv()
        for v in loc:
            v.wait()
        ss = jnp.zeros((tb, 1), F32)
        for k in range(8):
            v = xs[k].astype(F32)
            ss = ss + jnp.sum(v * v, axis=-1, keepdims=True)
        r = lax.rsqrt(ss / float(d) + EPS)
        for k in range(8):
            nb[:, dh * k:dh * (k + 1)] = (xs[k].astype(F32) * r * gb[k, 0:1, :]).astype(BF)
        part = (pl.ds(0, dc), pl.ds(dc, dc))
        yield from plane_ag(cn, p, lambda k: nb.at[:, part[k]], lambda zi, yi, k: n.at[zi, yi, :, part[k]],
                            lambda v, s: v.at[pl.ds(hb * s, hb), :], 13.0, 6.0, 16.0)

    tn = 256

    def gate_up(k, b):
        s, zh = b // 2, b % 2

        def step(t, carry):
            v = n[2 * zh:2 * zh + 2, :, hb * s:hb * (s + 1), :].reshape(8 * hb, d)
            cs = pl.ds(pl.multiple_of(cw[k][0] + t * tn, tn), tn)
            gt = _dot(v, wgb[:, :, cs].reshape(d, tn))
            up = _dot(v, wub[:, :, cs].reshape(d, tn))
            a1[b, :, cs] = (jax.nn.silu(gt) * up).astype(BF)
            return carry

        lax.fori_loop(0, cw[k][1] // tn, step, 0)
        got[k].append(cm.send(part_of(a1, b, k), part_of(a2, b, k), p.B))

    def first():
        yield from tokens()
        yield 47.5
        for wait in ready[0]:
            wait()
        for b in range(4):
            gate_up(0, b)
            yield 51.0 + 2.0 * b

    run(first(), weights())
    for wait in ready[1]:
        wait()
    for b in range(4):
        gate_up(1, b)
    for v in own:
        v.wait()
    cn.finish()

    qc = []
    m = p.x
    lo, hi, far = (m + 3) % 4, (m + 1) % 4, (m + 2) % 4

    def qweights():
        def blk(i):
            return wqb.at[2 * i + p.c]

        hr = wq.shape[0] // 2

        def half(i, s):
            return wqb.at[2 * i + p.c, pl.ds(hr * s, hr), :]

        p0 = cm.send(wq, blk(m), p.H(2))
        m0 = cm.send(wq, blk(m), p.H(-2))
        qc.append(cm.send(wq, blk(m), p.C))
        yield 112.0
        p0.wait_recv()
        p1 = cm.send(half(lo, 0), half(lo, 0), p.H(2))
        qc.append(cm.send(blk(lo), blk(lo), p.C))
        m0.wait_recv()
        m1 = cm.send(half(hi, 1), half(hi, 1), p.H(-2))
        qc.append(cm.send(blk(hi), blk(hi), p.C))
        yield 120.0
        p1.wait_recv()
        m1.wait_recv()
        qc.append(cm.send(blk(far), blk(far), p.C))
        yield 127.0
        for v in qc:
            v.wait_recv()

    kn = 512

    def down(b):
        s, zh = b // 2, b % 2
        for k in range(2):
            got[k][b].wait_recv()

        def step(t, carry):
            cs = dyn(t, kn)
            ob = ov[512 * zh:512 * (zh + 1), :].reshape(8, tb, -1)[:, hb * s:hb * (s + 1), :].reshape(8 * hb, -1)
            v = (_dot(a1[b], wdb[dyn(p.j, ww), cs]) + _dot(a2[b], wdb[dyn(1 - p.j, ww), cs]) + _dot(ob, wob[:, cs]))
            y[s, 2 * zh:2 * zh + 2, :, :, cs] = v.reshape(2, 4, hb, kn)
            return carry

        lax.fori_loop(0, wdb.shape[1] // kn, step, 0)

    xex = []

    def chain(s, t0):
        if s == 0:
            for k, (v, sl) in enumerate(down_in):
                yield 66.0 + 10.0 * k
                v.wait_recv()
                late.append(cm.send(sl, sl, p.C))
            yield 88.0
            for v in late:
                v.wait_recv()
        else:
            yield t0 - 8.0
        down(2 * s)
        yield t0 - 2.0
        down(2 * s + 1)
        ca, cb = pl.ds(0, dc // 2), pl.ds(dc // 2, dc // 2)

        def both(get_a, get_b, r, f, res_a, res_b, ax_a, ax_b, t, u):
            ga = ring_rs(cm, get_a, r.at[s, 0], r.at[s, 1], f.at[s, 0], f.at[s, 1], res_a, *ax_a, t, u)
            gb_ = ring_rs(cm, get_b, r.at[s, 2], r.at[s, 3], f.at[s, 2], f.at[s, 3], res_b, *ax_b, t, u)
            for v, _ in zip(ga, gb_):
                yield v
            list(gb_)

        def rr(k):
            return pl.ds(qb * k, qb)

        ay, az = (p.y, p.Y(1), p.Y(-1)), (p.z, p.Z(1), p.Z(-1))
        yield from both(lambda i, k: y.at[s, :, i, rr(k), ca], lambda i, k: y.at[s, i, :, rr(k), cb], r1, f1,
                        lambda k: y.at[s, :, p.y, rr(k), ca], lambda k: y.at[s, p.z, :, rr(k), cb], ay, az, t0 + 1.5, 8.5)
        yield from both(lambda i, k: y.at[s, i, p.y, rr(k), ca], lambda i, k: y.at[s, p.z, i, rr(k), cb], r2, f2,
                        lambda k: s2.at[s, 0, rr(k), :], lambda k: s2.at[s, 1, rr(k), :], az, ay, t0 + 14.5, 3.0)
        t = t0 + 20.0
        rs = pl.ds(hb * s, hb)
        for k in range(4):
            yk = s2[s, k // 2, :, dh * (k % 2):dh * (k % 2 + 1)]
            xn[s, :, dh * k:dh * (k + 1)] = (xs[4 * p.j + k, rs, :].astype(F32) + yk).astype(BF)
        ex = cm.send(xn.at[s, dyn(1 - p.j, qb), :], xr.at[s], p.B)
        for v in (p.A, p.C, p.AC):
            xex.append(cm.send(xn.at[s, :, dyn(v[1] % 4, dh)], xq.at[p.q, rs, :], v).wait_recv)
        xex.append(cm.local(xn.at[s, :, dyn(p.h % 4, dh)], xq.at[p.q, rs, :]).wait)
        mine = xn[s, dyn(p.j, qb), :].astype(F32)
        yield t + 2.0
        ex.wait_recv()
        oth = xr[s].astype(F32)
        ss = jnp.sum(mine * mine, axis=-1, keepdims=True) + jnp.sum(oth * oth, axis=-1, keepdims=True)
        r = lax.rsqrt(ss / float(d) + EPS)
        for k in range(4):
            cs = slice(dh * k, dh * (k + 1))
            nh[s, p.j, :, cs] = (mine[:, cs] * r * gb[4 * p.j + k, 1:2, :]).astype(BF)
            nh[s, 1 - p.j, :, cs] = (oth[:, cs] * r * gb[4 * (1 - p.j) + k, 1:2, :]).astype(BF)
        part = (pl.ds(0, dc), pl.ds(dc, dc))
        n1 = n.at[:, :, pl.ds(hb * s, qb), :]
        yield from plane_ag(cm, p, lambda k: nh.at[s, k], lambda zi, yi, k: n1.at[zi, yi, :, part[k]],
                            None, t + 3.0, 3.0, 6.0)
        yield t + 20.0

        if s == 0:
            for _ in qw:
                pass

        def proj(t_, carry):
            cs = dyn(t_, tn)
            qk[s, :, :, cs] = _dot(n[:, :, hb * s:hb * s + qb, :].reshape(16 * qb, d), wqb[:, :, cs].reshape(d, tn)).astype(BF).reshape(16, qb, tn)
            return carry

        lax.fori_loop(0, wq.shape[1] // tn, proj, 0)

        def blk(xx):
            h = 2 * xx + p.c
            return q_o.at[quarter(h), :, s, h // 4]

        def half(xx, k):
            h = 2 * xx + p.c
            return q_o.at[quarter(h), pl.ds(8 * k, 8), s, h // 4]

        own = cm.local(qk.at[s], blk(m))
        p0 = cm.send(qk.at[s], blk(m), p.H(2))
        m0 = cm.send(qk.at[s], blk(m), p.H(-2))
        c = [cm.send(qk.at[s], blk(m), p.C)]
        yield t + 31.0
        p0.wait_recv()
        p1 = cm.send(half(lo, 0), half(lo, 0), p.H(2))
        m0.wait_recv()
        m1 = cm.send(half(hi, 1), half(hi, 1), p.H(-2))
        for b in (blk(lo), blk(hi)):
            c.append(cm.send(b, b, p.C))
        yield t + 38.0
        p1.wait_recv()
        c.append(cm.send(half(far, 0), half(far, 0), p.C))
        m1.wait_recv()
        c.append(cm.send(half(far, 1), half(far, 1), p.C))
        yield t + 42.0
        own.wait()
        for v in c:
            v.wait_recv()

    def resid():
        yield 134.0
        for wait in xex:
            wait()
        yield from plane_ag(cm, p, lambda k: xq.at[pl.ds(2 * k, 2)], lambda zi, yi, k: x_o.at[pl.ds(2 * k, 2), zi, yi],
                            None, 134.0, 3.0, 10.0)

    def qrest():
        yield next(qw)
        yield from qw

    qw = qweights()
    run(qrest(), chain(0, 92.0), chain(1, 96.5), resid())
    cm.finish()


def solution(mesh):
    def body(x, g1, g2, w_gate, w_up, w_down, o, w_o, w_qkv):
        t, dh = x.shape
        d = dh * 8
        ff = w_gate.shape[1]
        tq = t // 4
        tb = tq // 16
        fh = ff // 2
        hb, qb, w2, nq = tb // 2, tb // 4, d // 4, w_qkv.shape[1]
        g = jnp.concatenate([jnp.stack([g1, g2]), jnp.zeros((6, dh), F32)], axis=0)
        bf, f32 = (lambda *v: pltpu.VMEM(v, BF)), (lambda *v: pltpu.VMEM(v, F32))
        ns = 216
        xo, qo = pl.pallas_call(
            block,
            out_shape=[jax.ShapeDtypeStruct((4, 4, 4, tb, dh), BF), jax.ShapeDtypeStruct((4, 16, 2, 2, qb, nq), BF)],
            in_specs=[HB] * 8,
            out_specs=[ANY] * 2,
            scratch_shapes=[
                bf(8, tb, dh), f32(8, 8, dh), bf(tb, d), bf(4, 4, tb, d), bf(8, dh, fh), bf(8, dh, fh),
                bf(ff, d // 2), bf(w_o.shape[0], d // 2), bf(8, dh, nq), bf(tq, w_o.shape[0]),
                bf(4, tq // 4, fh), bf(4, tq // 4, fh), f32(2, 4, 4, hb, d // 2),
                f32(2, 4, 4, qb, w2), f32(2, 4, 4, hb, w2), f32(2, 4, qb, w2), f32(2, 4, hb, w2), f32(2, 2, hb, w2),
                bf(2, hb, d // 2), bf(2, qb, d // 2), bf(2, 2, qb, d // 2), bf(2, 16, qb, nq),
                bf(4, tb, dh),
                pltpu.SemaphoreType.DMA((ns,)), pltpu.SemaphoreType.DMA((ns,)), pltpu.SemaphoreType.DMA((28,))],
            compiler_params=pltpu.CompilerParams(collective_id=1, has_side_effects=True,
                                                 vmem_limit_bytes=VLIM),
            name='block',
        )(x, g, w_gate, w_up, w_down, o, w_o, w_qkv)
        return xo.reshape(t, dh), qo.reshape(t, -1)

    in_specs = (P(None, 'h'), P('h'), P('h'), P('h', 'f'), P('h', 'f'), P('f', 'h'),
                P(None, 'f'), P('f', 'h'), P('h', 'f'))
    return jax.shard_map(body, mesh=mesh, in_specs=in_specs,
                         out_specs=(P(None, 'h'), P(None, 'f')), check_vma=False)
```

```python
import functools

import jax
import jax.numpy as jnp
from jax import lax
from jax.experimental import pallas as pl
from jax.experimental.pallas import tpu as pltpu
from jax.sharding import PartitionSpec as P

EPS = 1e-6
VLIM = 56 * 1024 * 1024
MESH = pl.DeviceIdType.MESH
ANY = pl.BlockSpec(memory_space=pl.ANY)
VM = pl.BlockSpec(memory_space=pltpu.VMEM)
HB = pl.BlockSpec(memory_space=pltpu.HBM)
BF = jnp.bfloat16
F32 = jnp.float32


def _dot(a, b):
    return jnp.dot(a, b, preferred_element_type=jnp.float32)


class Pos:
    def __init__(self):
        self.f = lax.axis_index('f')
        self.h = lax.axis_index('h')
        self.z, self.y = self.f // 4, self.f % 4
        self.x, self.c = self.h // 2, self.h % 2
        self.j = self.x // 2
        self.q = quarter(self.h)
        ax = self.x + 1 - 2 * (self.x % 2)
        self.A = (self.f, 2 * ax + self.c)
        self.B = (self.f, 2 * (3 - self.x) + self.c)
        self.C = (self.f, self.h + 1 - 2 * self.c)
        self.AC = (self.f, 2 * ax + 1 - self.c)

    def H(self, d):
        return (self.f, (self.h + d) % 8)

    def Y(self, d):
        return (4 * self.z + (self.y + d) % 4, self.h)

    def Z(self, d):
        return (4 * ((self.z + d) % 4) + self.y, self.h)


def quarter(h):
    x = h // 2
    return 2 * ((x + x // 2) % 2) + h % 2


class Comm:
    def __init__(self, ssem, rsem, lsem):
        self.ssem, self.rsem, self.lsem = ssem, rsem, lsem
        self.k = 0
        self.lk = 0
        self.sent = []

    def send(self, src, dst, dev):
        c = pltpu.make_async_remote_copy(src_ref=src, dst_ref=dst, send_sem=self.ssem.at[self.k],
                                         recv_sem=self.rsem.at[self.k], device_id=dev, device_id_type=MESH)
        self.k += 1
        c.start()
        self.sent.append(c)
        return c

    def local(self, src, dst):
        c = pltpu.make_async_copy(src, dst, self.lsem.at[self.lk])
        self.lk += 1
        c.start()
        return c

    def finish(self):
        for c in self.sent:
            c.wait_send()


class Part(Comm):
    def __init__(self, cm):
        self.cm = cm
        self.sent = []

    def send(self, src, dst, dev):
        c = self.cm.send(src, dst, dev)
        self.sent.append(self.cm.sent.pop())
        return c

    def local(self, src, dst):
        return self.cm.local(src, dst)


def barrier(devs):
    b = pltpu.get_barrier_semaphore()
    for d in devs:
        pl.semaphore_signal(b, inc=1, device_id=d, device_id_type=MESH)
    pl.semaphore_wait(b, len(devs))


def run(*gens):
    live = []
    for g in gens:
        t = next(g, None)
        if t is not None:
            live.append([t, g])
    while live:
        e = min(live, key=lambda v: v[0])
        t = next(e[1], None)
        if t is None:
            live.remove(e)
        else:
            e[0] = t


def ring_ag(cm, own, blk, half, m, plus, minus, t0, u):
    lo, hi = (m + 3) % 4, (m + 1) % 4
    p0 = cm.send(own, blk(m), plus)
    m0 = cm.send(own, blk(m), minus)
    yield t0 + u
    p0.wait_recv()
    p1 = cm.send(half(lo, 0), half(lo, 0), plus)
    m0.wait_recv()
    m1 = cm.send(half(hi, 1), half(hi, 1), minus)
    yield t0 + 1.5 * u
    p1.wait_recv()
    m1.wait_recv()


def ring_direct(cm, own, blk, m, sides, t0, u):
    c = [cm.send(own, blk(m), v) for v in sides]
    yield t0 + u
    for v in c:
        v.wait_recv()


def plane_ag(cm, p, own, n_o, half, t0, u1, u2):
    if half is None:
        ya = ring_direct(cm, own(0), lambda i: n_o(p.z, i, 0), p.y, (p.Y(1), p.Y(-1), p.Y(2)), t0, u1)
        zb = ring_direct(cm, own(1), lambda i: n_o(i, p.y, 1), p.z, (p.Z(1), p.Z(-1), p.Z(2)), t0, u1)
    else:
        ya = ring_ag(cm, own(0), lambda i: n_o(p.z, i, 0), lambda i, s: half(n_o(p.z, i, 0), s), p.y, p.Y(1), p.Y(-1), t0, u1)
        zb = ring_ag(cm, own(1), lambda i: n_o(i, p.y, 1), lambda i, s: half(n_o(i, p.y, 1), s), p.z, p.Z(1), p.Z(-1), t0, u1)
    loc = [cm.local(own(k), n_o(p.z, p.y, k)) for k in range(2)]
    for t, _ in zip(ya, zb):
        yield t
    list(zb)
    for v in loc:
        v.wait()
    t1 = t0 + (u1 if half is None else 1.5 * u1 + 2.0)
    al, h2 = slice(None), lambda s: pl.ds(2 * s, 2)
    za = ring_ag(cm, n_o(p.z, al, 0), lambda i: n_o(i, al, 0), lambda i, s: n_o(i, h2(s), 0), p.z, p.Z(1), p.Z(-1), t1, u2)
    yb = ring_ag(cm, n_o(al, p.y, 1), lambda i: n_o(al, i, 1), lambda i, s: n_o(h2(s), i, 1), p.y, p.Y(1), p.Y(-1), t1, u2)
    for t, _ in zip(za, yb):
        yield t
    list(yb)


def ring_rs(cm, get, r1p, r1m, fp, fm, res, m, plus, minus, t0, u, lat):
    lo, hi, far = (m + 3) % 4, (m + 1) % 4, (m + 2) % 4
    hb = r1p.shape[-2]
    f0, f1 = (Ellipsis, pl.ds(0, hb), slice(None)), (Ellipsis, pl.ds(hb, hb), slice(None))
    p0 = cm.send(get(far, 0), r1p, plus)
    m0 = cm.send(get(far, 1), r1m, minus)
    p1 = cm.send(get(hi, 1), fp.at[f1], plus)
    m1 = cm.send(get(lo, 0), fm.at[f0], minus)
    yield t0 + 0.5 * u + lat
    p0.wait_recv()
    v = get(hi, 0)
    v[...] = r1p[...] + v[...]
    p2 = cm.send(v, fp.at[f0], plus)
    m0.wait_recv()
    v = get(lo, 1)
    v[...] = r1m[...] + v[...]
    m2 = cm.send(v, fm.at[f1], minus)
    yield t0 + 1.5 * u + 2.0 * lat
    p1.wait_recv()
    m1.wait_recv()
    p2.wait_recv()
    m2.wait_recv()
    res(0)[...] = (fp[f0] + fm[f0]) + get(m, 0)[...]
    res(1)[...] = (fp[f1] + fm[f1]) + get(m, 1)[...]


def ring_rs_direct(cm, get, r, res, m, sides, t0, u):
    c = [cm.send(get((m + k + 1) % 4), r.at[k], v) for k, v in enumerate(sides)]
    yield t0 + u
    for v in c:
        v.wait_recv()
    res[...] = (r[0] + r[1]) + (r[2] + get(m)[...])


def block(x, g, wg, wu, wd, o, wo, wq, x_o, q_o,
          xs, gb, nb, n, wgb, wub, wdb, wob, wqb, ov, a1, a2, y,
          r1, f1, r2, s2, xn, xr, nh, qk, xq, ssem, rsem, lsem):
    p = Pos()
    cm = Comm(ssem, rsem, lsem)
    barrier([p.H(k) for k in range(1, 8)] + [p.Y(k) for k in range(1, 4)] + [p.Z(k) for k in range(1, 4)])
    tb, dh = xs.shape[1:]
    ww = wgb.shape[2]
    d = n.shape[3]
    dc = d // 2
    hb = tb // 2
    qb = hb // 2
    al = slice(None)

    def dyn(i, m):
        return pl.ds(pl.multiple_of(i * m, m), m)

    def rows(q):
        return x.at[pl.ds(pl.multiple_of(1024 * q + tb * p.f, tb), tb), :]

    xin = []
    for k in range(1, 8):
        t = p.H(k)
        xin.append(cm.send(rows(quarter(t[1])), xs.at[p.h], t))
        xin.append(cm.send(g, gb.at[p.h], t))
    loc = [cm.local(rows(p.q), xs.at[p.h]), cm.local(g, gb.at[p.h])]

    cw = ((0, 512), (512, 256))

    def cols(w, j, k):
        return w.at[:, pl.ds(pl.multiple_of(ww * j + cw[k][0], 128), cw[k][1])]

    def part_of(b, h, k):
        return b.at[h, :, pl.ds(*cw[k])]

    def slot(b, h):
        return b.at[:, dyn(h % 4, dh)]

    down_in, late, got, own = [], [], [[], []], []
    cn = Part(cm)
    ready = [[], []]

    def weights():
        ws = ((wg, wgb), (wu, wub))
        fb, fa, f2_ = [[], []], [[], []], [[], []]
        opp = 2 * (3 - p.A[1] // 2) + p.c

        def fan(k, to_b, to_a):
            for w, wb in ws:
                dst = part_of(wb, p.h, k)
                if to_b:
                    fb[k].append(cm.send(cols(w, 1 - p.j, k), dst, p.B))
                if to_a:
                    fa[k].append(cm.send(cols(w, p.j, k), dst, p.A))
                    ready[k].append(cm.send(cols(w, p.j, k), dst, p.C).wait_recv)
                    ready[k].append(cm.local(cols(w, p.j, k), dst).wait)

        def take(c, wb, h, k, onward):
            c.wait_recv()
            v = part_of(wb, h, k)
            if onward:
                f2_[k].append(cm.send(v, v, p.A))
            ready[k].append(cm.send(v, v, p.C).wait_recv)

        fan(0, True, True)
        fan(1, True, False)
        own.append(cm.local(o.at[pl.ds(pl.multiple_of(1024 * p.q, 1024), 1024), :], ov))
        for w, wb in ((wd, wdb), (wo, wob)):
            own.append(cm.local(w, slot(wb, p.h)))
        own.append(cm.local(wq, wqb.at[p.h]))
        for k in range(2):
            yield 14.0 + 8.0 * k
            take(fb[0][k], ws[k][1], p.B[1], 0, True)
            take(fa[0][k], ws[k][1], p.A[1], 0, False)
        fan(1, False, True)
        yield 31.0
        for k in range(2):
            take(fb[1][k], ws[k][1], p.B[1], 1, True)
        hk = wd.shape[0] // 2
        down_in.append((cm.send(wo, slot(wob, p.h), p.A), slot(wob, p.A[1])))
        late.append(cm.send(wo, slot(wob, p.h), p.C))
        for r in range(2):
            down_in.append((cm.send(wd.at[pl.ds(hk * r, hk), :], slot(wdb, p.h).at[pl.ds(hk * r, hk), :], p.A),
                            slot(wdb, p.A[1]).at[pl.ds(hk * r, hk), :]))
        late.append(cm.send(wd, slot(wdb, p.h), p.C))
        for k in range(2):
            yield 34.0 + 7.0 * k
            take(f2_[0][k], ws[k][1], opp, 0, False)
        yield 49.0
        for k in range(2):
            take(fa[1][k], ws[k][1], p.A[1], 1, False)
        for k in range(2):
            yield 56.0 + 4.5 * k
            take(f2_[1][k], ws[k][1], opp, 1, False)

    def tokens():
        yield 5.0
        for v in xin:
            v.wait_recv()
        for v in loc:
            v.wait()
        ss = jnp.zeros((tb, 1), F32)
        for k in range(8):
            v = xs[k].astype(F32)
            ss = ss + jnp.sum(v * v, axis=-1, keepdims=True)
        r = lax.rsqrt(ss / float(d) + EPS)
        for k in range(8):
            nb[:, dh * k:dh * (k + 1)] = (xs[k].astype(F32) * r * gb[k, 0:1, :]).astype(BF)
        part = (pl.ds(0, dc), pl.ds(dc, dc))
        yield from plane_ag(cn, p, lambda k: nb.at[:, part[k]], lambda zi, yi, k: n.at[zi, yi, :, part[k]],
                            lambda v, s: v.at[pl.ds(hb * s, hb), :], 13.0, 6.0, 16.0)

    tn = 256

    def gate_up(k, b):
        s, zh = b // 2, b % 2

        def step(t, carry):
            v = n[2 * zh:2 * zh + 2, :, hb * s:hb * (s + 1), :].reshape(8 * hb, d)
            cs = pl.ds(pl.multiple_of(cw[k][0] + t * tn, tn), tn)
            gt = _dot(v, wgb[:, :, cs].reshape(d, tn))
            up = _dot(v, wub[:, :, cs].reshape(d, tn))
            a1[b, :, cs] = (jax.nn.silu(gt) * up).astype(BF)
            return carry

        lax.fori_loop(0, cw[k][1] // tn, step, 0)
        got[k].append(cm.send(part_of(a1, b, k), part_of(a2, b, k), p.B))

    def first():
        yield from tokens()
        yield 47.5
        for wait in ready[0]:
            wait()
        for b in range(4):
            gate_up(0, b)
            yield 51.0 + 2.0 * b

    run(first(), weights())
    for wait in ready[1]:
        wait()
    for b in range(4):
        gate_up(1, b)
    for v in own:
        v.wait()
    cn.finish()

    qc = []
    m = p.x
    lo, hi, far = (m + 3) % 4, (m + 1) % 4, (m + 2) % 4

    def qweights():
        def blk(i):
            return wqb.at[2 * i + p.c]

        hr = wq.shape[0] // 2

        def half(i, s):
            return wqb.at[2 * i + p.c, pl.ds(hr * s, hr), :]

        p0 = cm.send(wq, blk(m), p.H(2))
        m0 = cm.send(wq, blk(m), p.H(-2))
        qc.append(cm.send(wq, blk(m), p.C))
        yield 112.0
        p0.wait_recv()
        p1 = cm.send(half(lo, 0), half(lo, 0), p.H(2))
        qc.append(cm.send(blk(lo), blk(lo), p.C))
        m0.wait_recv()
        m1 = cm.send(half(hi, 1), half(hi, 1), p.H(-2))
        qc.append(cm.send(blk(hi), blk(hi), p.C))
        yield 120.0
        p1.wait_recv()
        m1.wait_recv()
        qc.append(cm.send(blk(far), blk(far), p.C))
        yield 127.0
        for v in qc:
            v.wait_recv()

    w3 = wdb.shape[1] // 2
    w4 = w3 // 2
    odd = p.x % 2
    xex = []

    def down(b, e):
        s, zh = b // 2, b % 2
        if e == 0:
            for k in range(2):
                got[k][b].wait_recv()
        base = w3 * (odd if e == 0 else 1 - odd)

        def step(t, carry):
            cs = pl.ds(pl.multiple_of(base + t * tn, tn), tn)
            ob = ov[512 * zh:512 * (zh + 1), :].reshape(8, tb, -1)[:, hb * s:hb * (s + 1), :].reshape(8 * hb, -1)
            v = (_dot(a1[b], wdb[dyn(p.j, ww), cs]) + _dot(a2[b], wdb[dyn(1 - p.j, ww), cs]) + _dot(ob, wob[:, cs]))
            y[s, 2 * zh:2 * zh + 2, :, :, pl.ds(pl.multiple_of(w3 * e + t * tn, tn), tn)] = v.reshape(2, 4, hb, tn)
            return carry

        lax.fori_loop(0, w3 // tn, step, 0)

    def rr(k):
        return pl.ds(qb * k, qb)

    ay, az = (p.y, p.Y(1), p.Y(-1)), (p.z, p.Z(1), p.Z(-1))

    def scatter(s, e, t):
        ca, cb = pl.ds(w3 * e, w4), pl.ds(w3 * e + w4, w4)

        def both(get_a, get_b, r, f, res_a, res_b, ax_a, ax_b, t, u, v):
            ga = ring_rs(cm, get_a, r.at[s, e, 0], r.at[s, e, 1], f.at[s, e, 0], f.at[s, e, 1], res_a, *ax_a, t, u, v)
            gb_ = ring_rs(cm, get_b, r.at[s, e, 2], r.at[s, e, 3], f.at[s, e, 2], f.at[s, e, 3], res_b, *ax_b, t, u, v)
            for q, _ in zip(ga, gb_):
                yield q
            list(gb_)

        yield from both(lambda i, k: y.at[s, :, i, rr(k), ca], lambda i, k: y.at[s, i, :, rr(k), cb], r1, f1,
                        lambda k: y.at[s, :, p.y, rr(k), ca], lambda k: y.at[s, p.z, :, rr(k), cb], ay, az, t, 3.0, 2.0)
        y3, z3 = [p.Y(k) for k in (1, 2, 3)], [p.Z(k) for k in (1, 2, 3)]
        ga = ring_rs_direct(cm, lambda i: y.at[s, i, p.y, :, ca], r2.at[s, e, 0], s2.at[s, e, 0], p.z, z3, t + 11.0, 4.0)
        gb_ = ring_rs_direct(cm, lambda i: y.at[s, p.z, i, :, cb], r2.at[s, e, 1], s2.at[s, e, 1], p.y, y3, t + 11.0, 4.0)
        for q, _ in zip(ga, gb_):
            yield q
        list(gb_)

    def weights2():
        for k, (v, sl) in enumerate(down_in):
            yield (66.0, 75.0, 87.5)[k]
            v.wait_recv()
            late.append(cm.send(sl, sl, p.C))

    def own_part(s, t0):
        yield t0 - 2.0
        if s == 0:
            for v in late[:2]:
                v.wait_recv()
            del late[:2]
        down(2 * s, 0)
        yield t0
        down(2 * s + 1, 0)
        yield from scatter(s, 0, t0 + 1.0)

    def chain(s, t0):
        yield t0 - 2.0
        if s == 0:
            for v in late:
                v.wait_recv()
        down(2 * s, 1)
        down(2 * s + 1, 1)
        yield from scatter(s, 1, t0 + 1.0)
        for _ in owns[s]:
            pass
        t = t0 + 18.0
        rs = pl.ds(hb * s, hb)
        for e in range(2):
            for k in range(2):
                i = 2 * (odd if e == 0 else 1 - odd) + k
                xn[s, :, dyn(i, dh)] = (xs[4 * p.j + i, rs, :].astype(F32) + s2[s, e, k]).astype(BF)
        ex = cm.send(xn.at[s, dyn(1 - p.j, qb), :], xr.at[s], p.B)
        for v in (p.A, p.C, p.AC):
            xex.append(cm.send(xn.at[s, :, dyn(v[1] % 4, dh)], xq.at[p.q, rs, :], v).wait_recv)
        xex.append(cm.local(xn.at[s, :, dyn(p.h % 4, dh)], xq.at[p.q, rs, :]).wait)
        mine = xn[s, dyn(p.j, qb), :].astype(F32)
        yield t + 2.0
        ex.wait_recv()
        oth = xr[s].astype(F32)
        ss = jnp.sum(mine * mine, axis=-1, keepdims=True) + jnp.sum(oth * oth, axis=-1, keepdims=True)
        r = lax.rsqrt(ss / float(d) + EPS)
        for k in range(4):
            cs = slice(dh * k, dh * (k + 1))
            nh[s, p.j, :, cs] = (mine[:, cs] * r * gb[4 * p.j + k, 1:2, :]).astype(BF)
            nh[s, 1 - p.j, :, cs] = (oth[:, cs] * r * gb[4 * (1 - p.j) + k, 1:2, :]).astype(BF)
        part = (pl.ds(0, dc), pl.ds(dc, dc))
        n1 = n.at[:, :, pl.ds(hb * s, qb), :]
        yield from plane_ag(cm, p, lambda k: nh.at[s, k], lambda zi, yi, k: n1.at[zi, yi, :, part[k]],
                            None, t + 3.0, 3.0, 6.0)
        yield t + 20.0

        if s == 0:
            for _ in qw:
                pass

        def proj(t_, carry):
            cs = dyn(t_, tn)
            qk[s, :, :, cs] = _dot(n[:, :, hb * s:hb * s + qb, :].reshape(16 * qb, d), wqb[:, :, cs].reshape(d, tn)).astype(BF).reshape(16, qb, tn)
            return carry

        lax.fori_loop(0, wq.shape[1] // tn, proj, 0)

        def blk(xx):
            h = 2 * xx + p.c
            return q_o.at[quarter(h), :, s, h // 4]

        def half(xx, k):
            h = 2 * xx + p.c
            return q_o.at[quarter(h), pl.ds(8 * k, 8), s, h // 4]

        own = cm.local(qk.at[s], blk(m))
        p0 = cm.send(qk.at[s], blk(m), p.H(2))
        m0 = cm.send(qk.at[s], blk(m), p.H(-2))
        c = [cm.send(qk.at[s], blk(m), p.C)]
        yield t + 31.0
        p0.wait_recv()
        p1 = cm.send(half(lo, 0), half(lo, 0), p.H(2))
        m0.wait_recv()
        m1 = cm.send(half(hi, 1), half(hi, 1), p.H(-2))
        for b in (blk(lo), blk(hi)):
            c.append(cm.send(b, b, p.C))
        yield t + 38.0
        p1.wait_recv()
        c.append(cm.send(half(far, 0), half(far, 0), p.C))
        m1.wait_recv()
        c.append(cm.send(half(far, 1), half(far, 1), p.C))
        yield t + 42.0
        own.wait()
        for v in c:
            v.wait_recv()

    def resid():
        yield 134.0
        for wait in xex:
            wait()
        yield from plane_ag(cm, p, lambda k: xq.at[pl.ds(2 * k, 2)], lambda zi, yi, k: x_o.at[pl.ds(2 * k, 2), zi, yi],
                            None, 134.0, 3.0, 10.0)

    def qrest():
        yield next(qw)
        yield from qw

    qw = qweights()
    owns = [own_part(0, 79.0), own_part(1, 85.0)]
    run(qrest(), weights2(), owns[0], owns[1], chain(0, 92.0), chain(1, 96.0), resid())
    cm.finish()


def solution(mesh):
    def body(x, g1, g2, w_gate, w_up, w_down, o, w_o, w_qkv):
        t, dh = x.shape
        d = dh * 8
        ff = w_gate.shape[1]
        tq = t // 4
        tb = tq // 16
        fh = ff // 2
        hb, qb, w2, nq = tb // 2, tb // 4, d // 4, w_qkv.shape[1]
        g = jnp.concatenate([jnp.stack([g1, g2]), jnp.zeros((6, dh), F32)], axis=0)
        bf, f32 = (lambda *v: pltpu.VMEM(v, BF)), (lambda *v: pltpu.VMEM(v, F32))
        ns = 232
        xo, qo = pl.pallas_call(
            block,
            out_shape=[jax.ShapeDtypeStruct((4, 4, 4, tb, dh), BF), jax.ShapeDtypeStruct((4, 16, 2, 2, qb, nq), BF)],
            in_specs=[HB] * 8,
            out_specs=[ANY] * 2,
            scratch_shapes=[
                bf(8, tb, dh), f32(8, 8, dh), bf(tb, d), bf(4, 4, tb, d), bf(8, dh, fh), bf(8, dh, fh),
                bf(ff, d // 2), bf(w_o.shape[0], d // 2), bf(8, dh, nq), bf(tq, w_o.shape[0]),
                bf(4, tq // 4, fh), bf(4, tq // 4, fh), f32(2, 4, 4, hb, d // 2),
                f32(2, 2, 4, 4, qb, w2 // 2), f32(2, 2, 4, 4, hb, w2 // 2), f32(2, 2, 2, 3, hb, w2 // 2),
                f32(2, 2, 2, hb, w2 // 2),
                bf(2, hb, d // 2), bf(2, qb, d // 2), bf(2, 2, qb, d // 2), bf(2, 16, qb, nq),
                bf(4, tb, dh),
                pltpu.SemaphoreType.DMA((ns,)), pltpu.SemaphoreType.DMA((ns,)), pltpu.SemaphoreType.DMA((28,))],
            compiler_params=pltpu.CompilerParams(collective_id=1, has_side_effects=True,
                                                 vmem_limit_bytes=VLIM),
            name='block',
        )(x, g, w_gate, w_up, w_down, o, w_o, w_qkv)
        return xo.reshape(t, dh), qo.reshape(t, -1)

    in_specs = (P(None, 'h'), P('h'), P('h'), P('h', 'f'), P('h', 'f'), P('f', 'h'),
                P(None, 'f'), P('f', 'h'), P('h', 'f'))
    return jax.shard_map(body, mesh=mesh, in_specs=in_specs,
                         out_specs=(P(None, 'h'), P(None, 'f')), check_vma=False)
```

```python
import functools

import jax
import jax.numpy as jnp
from jax import lax
from jax.experimental import pallas as pl
from jax.experimental.pallas import tpu as pltpu
from jax.sharding import PartitionSpec as P

EPS = 1e-6
VLIM = 56 * 1024 * 1024
MESH = pl.DeviceIdType.MESH
ANY = pl.BlockSpec(memory_space=pl.ANY)
VM = pl.BlockSpec(memory_space=pltpu.VMEM)
HB = pl.BlockSpec(memory_space=pltpu.HBM)
BF = jnp.bfloat16
F32 = jnp.float32


def _dot(a, b):
    return jnp.dot(a, b, preferred_element_type=jnp.float32)


class Pos:
    def __init__(self):
        self.f = lax.axis_index('f')
        self.h = lax.axis_index('h')
        self.z, self.y = self.f // 4, self.f % 4
        self.x, self.c = self.h // 2, self.h % 2
        self.j = self.x // 2
        self.q = quarter(self.h)
        ax = self.x + 1 - 2 * (self.x % 2)
        self.A = (self.f, 2 * ax + self.c)
        self.B = (self.f, 2 * (3 - self.x) + self.c)
        self.C = (self.f, self.h + 1 - 2 * self.c)
        self.AC = (self.f, 2 * ax + 1 - self.c)

    def H(self, d):
        return (self.f, (self.h + d) % 8)

    def Y(self, d):
        return (4 * self.z + (self.y + d) % 4, self.h)

    def Z(self, d):
        return (4 * ((self.z + d) % 4) + self.y, self.h)


def quarter(h):
    x = h // 2
    return 2 * ((x + x // 2) % 2) + h % 2


class Comm:
    def __init__(self, ssem, rsem, lsem):
        self.ssem, self.rsem, self.lsem = ssem, rsem, lsem
        self.k = 0
        self.lk = 0
        self.sent = []

    def send(self, src, dst, dev):
        c = pltpu.make_async_remote_copy(src_ref=src, dst_ref=dst, send_sem=self.ssem.at[self.k],
                                         recv_sem=self.rsem.at[self.k], device_id=dev, device_id_type=MESH)
        self.k += 1
        c.start()
        self.sent.append(c)
        return c

    def local(self, src, dst):
        c = pltpu.make_async_copy(src, dst, self.lsem.at[self.lk])
        self.lk += 1
        c.start()
        return c

    def finish(self):
        for c in self.sent:
            c.wait_send()


class Part(Comm):
    def __init__(self, cm):
        self.cm = cm
        self.sent = []

    def send(self, src, dst, dev):
        c = self.cm.send(src, dst, dev)
        self.sent.append(self.cm.sent.pop())
        return c

    def local(self, src, dst):
        return self.cm.local(src, dst)


def barrier(devs):
    b = pltpu.get_barrier_semaphore()
    for d in devs:
        pl.semaphore_signal(b, inc=1, device_id=d, device_id_type=MESH)
    pl.semaphore_wait(b, len(devs))


def run(*gens):
    live = []
    for g in gens:
        t = next(g, None)
        if t is not None:
            live.append([t, g])
    while live:
        e = min(live, key=lambda v: v[0])
        t = next(e[1], None)
        if t is None:
            live.remove(e)
        else:
            e[0] = t


def ring_ag(cm, own, blk, half, m, plus, minus, t0, u):
    lo, hi = (m + 3) % 4, (m + 1) % 4
    p0 = cm.send(own, blk(m), plus)
    m0 = cm.send(own, blk(m), minus)
    yield t0 + u
    p0.wait_recv()
    p1 = cm.send(half(lo, 0), half(lo, 0), plus)
    m0.wait_recv()
    m1 = cm.send(half(hi, 1), half(hi, 1), minus)
    yield t0 + 1.5 * u
    p1.wait_recv()
    m1.wait_recv()


def ring_direct(cm, own, blk, m, sides, t0, u):
    c = [cm.send(own, blk(m), v) for v in sides]
    yield t0 + u
    for v in c:
        v.wait_recv()


def plane_ag(cm, p, own, n_o, half, t0, u1, u2):
    if half is None:
        ya = ring_direct(cm, own(0), lambda i: n_o(p.z, i, 0), p.y, (p.Y(1), p.Y(-1), p.Y(2)), t0, u1)
        zb = ring_direct(cm, own(1), lambda i: n_o(i, p.y, 1), p.z, (p.Z(1), p.Z(-1), p.Z(2)), t0, u1)
    else:
        ya = ring_ag(cm, own(0), lambda i: n_o(p.z, i, 0), lambda i, s: half(n_o(p.z, i, 0), s), p.y, p.Y(1), p.Y(-1), t0, u1)
        zb = ring_ag(cm, own(1), lambda i: n_o(i, p.y, 1), lambda i, s: half(n_o(i, p.y, 1), s), p.z, p.Z(1), p.Z(-1), t0, u1)
    loc = [cm.local(own(k), n_o(p.z, p.y, k)) for k in range(2)]
    for t, _ in zip(ya, zb):
        yield t
    list(zb)
    for v in loc:
        v.wait()
    t1 = t0 + (u1 if half is None else 1.5 * u1 + 2.0)
    al, h2 = slice(None), lambda s: pl.ds(2 * s, 2)
    za = ring_ag(cm, n_o(p.z, al, 0), lambda i: n_o(i, al, 0), lambda i, s: n_o(i, h2(s), 0), p.z, p.Z(1), p.Z(-1), t1, u2)
    yb = ring_ag(cm, n_o(al, p.y, 1), lambda i: n_o(al, i, 1), lambda i, s: n_o(h2(s), i, 1), p.y, p.Y(1), p.Y(-1), t1, u2)
    for t, _ in zip(za, yb):
        yield t
    list(yb)


def ring_rs(cm, get, r1p, r1m, fp, fm, res, m, plus, minus, t0, t1):
    lo, hi, far = (m + 3) % 4, (m + 1) % 4, (m + 2) % 4
    hb = r1p.shape[-2]
    f0, f1 = (Ellipsis, pl.ds(0, hb), slice(None)), (Ellipsis, pl.ds(hb, hb), slice(None))
    p0 = cm.send(get(far, 0), r1p, plus)
    m0 = cm.send(get(far, 1), r1m, minus)
    p1 = cm.send(get(hi, 1), fp.at[f1], plus)
    m1 = cm.send(get(lo, 0), fm.at[f0], minus)
    yield t0
    p0.wait_recv()
    v = get(hi, 0)
    v[...] = r1p[...] + v[...]
    p2 = cm.send(v, fp.at[f0], plus)
    m0.wait_recv()
    v = get(lo, 1)
    v[...] = r1m[...] + v[...]
    m2 = cm.send(v, fm.at[f1], minus)
    yield t1
    p1.wait_recv()
    m1.wait_recv()
    p2.wait_recv()
    m2.wait_recv()
    res(0)[...] = (fp[f0] + fm[f0]) + get(m, 0)[...]
    res(1)[...] = (fp[f1] + fm[f1]) + get(m, 1)[...]


def ring_rs_direct(cm, get, r, res, m, sides, t0, u):
    c = [cm.send(get((m + k + 1) % 4), r.at[k], v) for k, v in enumerate(sides)]
    yield t0 + u
    for v in c:
        v.wait_recv()
    res[...] = (r[0] + r[1]) + (r[2] + get(m)[...])


def block(x, g, wg, wu, wd, o, wo, wq, x_o, q_o,
          xs, gb, nb, n, wgb, wub, wdb, wob, wqb, ov, a1, a2, y,
          r1, f1, r2, s2, xn, xr, nh, qk, xq, ssem, rsem, lsem):
    p = Pos()
    cm = Comm(ssem, rsem, lsem)
    barrier([p.H(k) for k in range(1, 8)] + [p.Y(k) for k in range(1, 4)] + [p.Z(k) for k in range(1, 4)])
    tb, dh = xs.shape[1:]
    ww = wgb.shape[2]
    d = n.shape[3]
    dc = d // 2
    hb = tb // 2
    qb = hb // 2
    al = slice(None)

    def dyn(i, m):
        return pl.ds(pl.multiple_of(i * m, m), m)

    def rows(q):
        return x.at[pl.ds(pl.multiple_of(1024 * q + tb * p.f, tb), tb), :]

    xin = []
    for k in range(1, 8):
        t = p.H(k)
        xin.append(cm.send(rows(quarter(t[1])), xs.at[p.h], t))
        xin.append(cm.send(g, gb.at[p.h], t))
    loc = [cm.local(rows(p.q), xs.at[p.h]), cm.local(g, gb.at[p.h])]

    cw = ((0, 512), (512, 256))

    def cols(w, j, k):
        return w.at[:, pl.ds(pl.multiple_of(ww * j + cw[k][0], 128), cw[k][1])]

    def part_of(b, h, k):
        return b.at[h, :, pl.ds(*cw[k])]

    def slot(b, h):
        return b.at[:, dyn(h % 4, dh)]

    down_in, late, got, own = [], [], [[], []], []
    cn = Part(cm)
    ready = [[], []]

    def weights():
        ws = ((wg, wgb), (wu, wub))
        fb, fa, f2_ = [[], []], [[], []], [[], []]
        opp = 2 * (3 - p.A[1] // 2) + p.c

        def fan(k, to_b, to_a):
            for w, wb in ws:
                dst = part_of(wb, p.h, k)
                if to_b:
                    fb[k].append(cm.send(cols(w, 1 - p.j, k), dst, p.B))
                if to_a:
                    fa[k].append(cm.send(cols(w, p.j, k), dst, p.A))
                    ready[k].append(cm.send(cols(w, p.j, k), dst, p.C).wait_recv)
                    ready[k].append(cm.local(cols(w, p.j, k), dst).wait)

        def take(c, wb, h, k, onward):
            c.wait_recv()
            v = part_of(wb, h, k)
            if onward:
                f2_[k].append(cm.send(v, v, p.A))
            ready[k].append(cm.send(v, v, p.C).wait_recv)

        fan(0, True, True)
        fan(1, True, False)
        own.append(cm.local(o.at[pl.ds(pl.multiple_of(1024 * p.q, 1024), 1024), :], ov))
        for w, wb in ((wd, wdb), (wo, wob)):
            own.append(cm.local(w, slot(wb, p.h)))
        own.append(cm.local(wq, wqb.at[p.h]))
        for k in range(2):
            yield 14.0 + 8.0 * k
            take(fb[0][k], ws[k][1], p.B[1], 0, True)
            take(fa[0][k], ws[k][1], p.A[1], 0, False)
        fan(1, False, True)
        yield 31.0
        for k in range(2):
            take(fb[1][k], ws[k][1], p.B[1], 1, True)
        hk = wd.shape[0] // 2
        down_in.append((cm.send(wo, slot(wob, p.h), p.A), slot(wob, p.A[1])))
        late.append(cm.send(wo, slot(wob, p.h), p.C))
        for r in range(2):
            down_in.append((cm.send(wd.at[pl.ds(hk * r, hk), :], slot(wdb, p.h).at[pl.ds(hk * r, hk), :], p.A),
                            slot(wdb, p.A[1]).at[pl.ds(hk * r, hk), :]))
        late.append(cm.send(wd, slot(wdb, p.h), p.C))
        for k in range(2):
            yield 34.0 + 7.0 * k
            take(f2_[0][k], ws[k][1], opp, 0, False)
        yield 49.0
        for k in range(2):
            take(fa[1][k], ws[k][1], p.A[1], 1, False)
        for k in range(2):
            yield 56.0 + 4.5 * k
            take(f2_[1][k], ws[k][1], opp, 1, False)

    def tokens():
        yield 5.0
        for v in xin:
            v.wait_recv()
        for v in loc:
            v.wait()
        ss = jnp.zeros((tb, 1), F32)
        for k in range(8):
            v = xs[k].astype(F32)
            ss = ss + jnp.sum(v * v, axis=-1, keepdims=True)
        r = lax.rsqrt(ss / float(d) + EPS)
        for k in range(8):
            for i in range(dh // 128):
                ls = slice(128 * i, 128 * (i + 1))
                nb[:, dh * k + 128 * i:dh * k + 128 * (i + 1)] = (xs[k, :, ls].astype(F32) * r * gb[k, i:i + 1, :]).astype(BF)
        part = (pl.ds(0, dc), pl.ds(dc, dc))
        yield from plane_ag(cn, p, lambda k: nb.at[:, part[k]], lambda zi, yi, k: n.at[zi, yi, :, part[k]],
                            lambda v, s: v.at[pl.ds(hb * s, hb), :], 13.0, 6.0, 16.0)

    tn = 256

    def gate_up(k, b):
        s, zh = b // 2, b % 2

        def step(t, carry):
            v = n[2 * zh:2 * zh + 2, :, hb * s:hb * (s + 1), :].reshape(8 * hb, d)
            cs = pl.ds(pl.multiple_of(cw[k][0] + t * tn, tn), tn)
            gt = _dot(v, wgb[:, :, cs].reshape(d, tn))
            up = _dot(v, wub[:, :, cs].reshape(d, tn))
            a1[b, :, cs] = (jax.nn.silu(gt) * up).astype(BF)
            return carry

        lax.fori_loop(0, cw[k][1] // tn, step, 0)
        got[k].append(cm.send(part_of(a1, b, k), part_of(a2, b, k), p.B))

    def first():
        yield from tokens()
        yield 47.5
        for wait in ready[0]:
            wait()
        for b in range(4):
            gate_up(0, b)
            yield 51.0 + 2.0 * b

    run(first(), weights())
    for wait in ready[1]:
        wait()
    for b in range(4):
        gate_up(1, b)
    for v in own:
        v.wait()
    cn.finish()

    qc = []
    m = p.x
    lo, hi, far = (m + 3) % 4, (m + 1) % 4, (m + 2) % 4

    def qweights():
        def blk(i):
            return wqb.at[2 * i + p.c]

        hr = wq.shape[0] // 2

        def half(i, s):
            return wqb.at[2 * i + p.c, pl.ds(hr * s, hr), :]

        p0 = cm.send(wq, blk(m), p.H(2))
        m0 = cm.send(wq, blk(m), p.H(-2))
        qc.append(cm.send(wq, blk(m), p.C))
        yield 104.0
        p0.wait_recv()
        p1 = cm.send(half(lo, 0), half(lo, 0), p.H(2))
        qc.append(cm.send(blk(lo), blk(lo), p.C))
        m0.wait_recv()
        m1 = cm.send(half(hi, 1), half(hi, 1), p.H(-2))
        qc.append(cm.send(blk(hi), blk(hi), p.C))
        yield 111.5
        p1.wait_recv()
        m1.wait_recv()
        qc.append(cm.send(blk(far), blk(far), p.C))
        yield 115.0
        for v in qc:
            v.wait_recv()

    w3 = wdb.shape[1] // 2
    w4 = w3 // 2
    odd = p.x % 2
    xex = []

    def down(b, e):
        s, zh = b // 2, b % 2
        if e == 0:
            for k in range(2):
                got[k][b].wait_recv()
        base = w3 * (odd if e == 0 else 1 - odd)

        def step(t, carry):
            cs = pl.ds(pl.multiple_of(base + t * tn, tn), tn)
            ob = ov[512 * zh:512 * (zh + 1), :].reshape(8, tb, -1)[:, hb * s:hb * (s + 1), :].reshape(8 * hb, -1)
            v = (_dot(a1[b], wdb[dyn(p.j, ww), cs]) + _dot(a2[b], wdb[dyn(1 - p.j, ww), cs]) + _dot(ob, wob[:, cs]))
            y[s, 2 * zh:2 * zh + 2, :, :, pl.ds(pl.multiple_of(w3 * e + t * tn, tn), tn)] = v.reshape(2, 4, hb, tn)
            return carry

        lax.fori_loop(0, w3 // tn, step, 0, unroll=True)

    def rr(k):
        return pl.ds(qb * k, qb)

    ay, az = (p.y, p.Y(1), p.Y(-1)), (p.z, p.Z(1), p.Z(-1))

    def scatter(s, e, t0, t1, t2):
        ca, cb = pl.ds(w3 * e, w4), pl.ds(w3 * e + w4, w4)

        def both(get_a, get_b, r, f, res_a, res_b, ax_a, ax_b):
            ga = ring_rs(cm, get_a, r.at[s, e, 0], r.at[s, e, 1], f.at[s, e, 0], f.at[s, e, 1], res_a, *ax_a, t0, t1)
            gb_ = ring_rs(cm, get_b, r.at[s, e, 2], r.at[s, e, 3], f.at[s, e, 2], f.at[s, e, 3], res_b, *ax_b, t0, t1)
            for q, _ in zip(ga, gb_):
                yield q
            list(gb_)

        yield from both(lambda i, k: y.at[s, :, i, rr(k), ca], lambda i, k: y.at[s, i, :, rr(k), cb], r1, f1,
                        lambda k: y.at[s, :, p.y, rr(k), ca], lambda k: y.at[s, p.z, :, rr(k), cb], ay, az)
        y3, z3 = [p.Y(k) for k in (1, 2, 3)], [p.Z(k) for k in (1, 2, 3)]
        ga = ring_rs_direct(cm, lambda i: y.at[s, i, p.y, :, ca], r2.at[s, e, 0], s2.at[s, e, 0], p.z, z3, t2, 0.0)
        gb_ = ring_rs_direct(cm, lambda i: y.at[s, p.z, i, :, cb], r2.at[s, e, 1], s2.at[s, e, 1], p.y, y3, t2, 0.0)
        for q, _ in zip(ga, gb_):
            yield q
        list(gb_)

    def weights2():
        for k, (v, sl) in enumerate(down_in):
            yield (66.0, 74.0, 86.3)[k]
            v.wait_recv()
            late.append(cm.send(sl, sl, p.C))

    def own_part(s, t0, t):
        yield t0 - 2.0
        if s == 0:
            for v in late[:2]:
                v.wait_recv()
            del late[:2]
        down(2 * s, 0)
        yield t0
        down(2 * s + 1, 0)
        yield from scatter(s, 0, *t)

    def chain(s, t0, dt, t):
        yield t0 - 2.0
        if s == 0:
            for v in late:
                v.wait_recv()
        down(2 * s, 1)
        down(2 * s + 1, 1)
        yield from scatter(s, 1, *t)
        for _ in owns[s]:
            pass
        t = t0 + 14.5 + dt
        rs = pl.ds(hb * s, hb)
        for e in range(2):
            for k in range(2):
                i = 2 * (odd if e == 0 else 1 - odd) + k
                xn[s, :, dyn(i, dh)] = (xs[4 * p.j + i, rs, :].astype(F32) + s2[s, e, k]).astype(BF)
        ex = cm.send(xn.at[s, dyn(1 - p.j, qb), :], xr.at[s], p.B)
        for v in (p.A, p.C, p.AC):
            xex.append(cm.send(xn.at[s, :, dyn(v[1] % 4, dh)], xq.at[p.q, rs, :], v).wait_recv)
        xex.append(cm.local(xn.at[s, :, dyn(p.h % 4, dh)], xq.at[p.q, rs, :]).wait)
        mine = xn[s, dyn(p.j, qb), :].astype(F32)
        yield t + 2.0
        ex.wait_recv()
        oth = xr[s].astype(F32)
        ss = jnp.sum(mine * mine, axis=-1, keepdims=True) + jnp.sum(oth * oth, axis=-1, keepdims=True)
        r = lax.rsqrt(ss / float(d) + EPS)
        ng = dh // 128
        for k in range(4):
            for i in range(ng):
                cs = slice(dh * k + 128 * i, dh * k + 128 * (i + 1))
                gs = slice(ng + i, ng + i + 1)
                nh[s, p.j, :, cs] = (mine[:, cs] * r * gb[4 * p.j + k, gs, :]).astype(BF)
                nh[s, 1 - p.j, :, cs] = (oth[:, cs] * r * gb[4 * (1 - p.j) + k, gs, :]).astype(BF)
        part = (pl.ds(0, dc), pl.ds(dc, dc))
        n1 = n.at[:, :, pl.ds(hb * s, qb), :]
        yield from plane_ag(cm, p, lambda k: nh.at[s, k], lambda zi, yi, k: n1.at[zi, yi, :, part[k]],
                            None, t + 3.0, 3.0, 6.0)
        yield t + 15.5

        if s == 0:
            for _ in qw:
                pass

        def proj(t_, carry):
            cs = dyn(t_, tn)
            qk[s, :, :, cs] = _dot(n[:, :, hb * s:hb * s + qb, :].reshape(16 * qb, d), wqb[:, :, cs].reshape(d, tn)).astype(BF).reshape(16, qb, tn)
            return carry

        lax.fori_loop(0, wq.shape[1] // tn, proj, 0, unroll=True)

        def blk(xx):
            h = 2 * xx + p.c
            return q_o.at[quarter(h), :, s, h // 4]

        def half(xx, k):
            h = 2 * xx + p.c
            return q_o.at[quarter(h), pl.ds(8 * k, 8), s, h // 4]

        own = cm.local(qk.at[s], blk(m))
        p0 = cm.send(qk.at[s], blk(m), p.H(2))
        m0 = cm.send(qk.at[s], blk(m), p.H(-2))
        c = [cm.send(qk.at[s], blk(m), p.C)]
        yield t + 26.0 + 1.75 * dt
        p0.wait_recv()
        p1 = cm.send(half(lo, 0), half(lo, 0), p.H(2))
        m0.wait_recv()
        m1 = cm.send(half(hi, 1), half(hi, 1), p.H(-2))
        for b in (blk(lo), blk(hi)):
            c.append(cm.send(b, b, p.C))
        yield t + 32.0 + 1.75 * dt
        p1.wait_recv()
        c.append(cm.send(half(far, 0), half(far, 0), p.C))
        m1.wait_recv()
        c.append(cm.send(half(far, 1), half(far, 1), p.C))
        yield t + 35.0 + 1.75 * dt
        own.wait()
        for v in c:
            v.wait_recv()

    def resid():
        yield 130.5
        for wait in xex:
            wait()
        yield from plane_ag(cm, p, lambda k: xq.at[pl.ds(2 * k, 2)], lambda zi, yi, k: x_o.at[pl.ds(2 * k, 2), zi, yi],
                            None, 131.5, 4.0, 10.0)

    def qrest():
        yield 89.0
        yield next(qw)
        yield from qw

    qw = qweights()
    owns = [own_part(0, 75.0, (81.0, 86.0, 90.0)), own_part(1, 81.0, (87.0, 100.5, 104.0))]
    run(qrest(), weights2(), owns[0], owns[1], chain(0, 92.0, 0.0, (97.3, 102.3, 106.3)), chain(1, 94.6, 4.0, (99.9, 104.9, 108.9)), resid())
    cm.finish()


def solution(mesh):
    def body(x, g1, g2, w_gate, w_up, w_down, o, w_o, w_qkv):
        t, dh = x.shape
        d = dh * 8
        ff = w_gate.shape[1]
        tq = t // 4
        tb = tq // 16
        fh = ff // 2
        hb, qb, w2, nq = tb // 2, tb // 4, d // 4, w_qkv.shape[1]
        g = jnp.concatenate([g1, g2]).reshape(2 * dh // 128, 128)
        bf, f32 = (lambda *v: pltpu.VMEM(v, BF)), (lambda *v: pltpu.VMEM(v, F32))
        ns = 232
        xo, qo = pl.pallas_call(
            block,
            out_shape=[jax.ShapeDtypeStruct((4, 4, 4, tb, dh), BF), jax.ShapeDtypeStruct((4, 16, 2, 2, qb, nq), BF)],
            in_specs=[HB] * 8,
            out_specs=[ANY] * 2,
            scratch_shapes=[
                bf(8, tb, dh), f32(8, 2 * dh // 128, 128), bf(tb, d), bf(4, 4, tb, d), bf(8, dh, fh), bf(8, dh, fh),
                bf(ff, d // 2), bf(w_o.shape[0], d // 2), bf(8, dh, nq), bf(tq, w_o.shape[0]),
                bf(4, tq // 4, fh), bf(4, tq // 4, fh), f32(2, 4, 4, hb, d // 2),
                f32(2, 2, 4, 4, qb, w2 // 2), f32(2, 2, 4, 4, hb, w2 // 2), f32(2, 2, 2, 3, hb, w2 // 2),
                f32(2, 2, 2, hb, w2 // 2),
                bf(2, hb, d // 2), bf(2, qb, d // 2), bf(2, 2, qb, d // 2), bf(2, 16, qb, nq),
                bf(4, tb, dh),
                pltpu.SemaphoreType.DMA((ns,)), pltpu.SemaphoreType.DMA((ns,)), pltpu.SemaphoreType.DMA((28,))],
            compiler_params=pltpu.CompilerParams(collective_id=1, has_side_effects=True,
                                                 vmem_limit_bytes=VLIM),
            name='block',
        )(x, g, w_gate, w_up, w_down, o, w_o, w_qkv)
        return xo.reshape(t, dh), qo.reshape(t, -1)

    in_specs = (P(None, 'h'), P('h'), P('h'), P('h', 'f'), P('h', 'f'), P('f', 'h'),
                P(None, 'f'), P('f', 'h'), P('h', 'f'))
    return jax.shard_map(body, mesh=mesh, in_specs=in_specs,
                         out_specs=(P(None, 'h'), P(None, 'f')), check_vma=False)
```

```python
import functools

import jax
import jax.numpy as jnp
from jax import lax
from jax.experimental import pallas as pl
from jax.experimental.pallas import tpu as pltpu
from jax.sharding import PartitionSpec as P

EPS = 1e-6
VLIM = 56 * 1024 * 1024
MESH = pl.DeviceIdType.MESH
ANY = pl.BlockSpec(memory_space=pl.ANY)
VM = pl.BlockSpec(memory_space=pltpu.VMEM)
HB = pl.BlockSpec(memory_space=pltpu.HBM)
BF = jnp.bfloat16
F32 = jnp.float32


def _dot(a, b):
    return jnp.dot(a, b, preferred_element_type=jnp.float32)


class Pos:
    def __init__(self):
        self.f = lax.axis_index('f')
        self.h = lax.axis_index('h')
        self.z, self.y = self.f // 4, self.f % 4
        self.x, self.c = self.h // 2, self.h % 2
        self.j = self.x // 2
        self.q = quarter(self.h)
        ax = self.x + 1 - 2 * (self.x % 2)
        self.A = (self.f, 2 * ax + self.c)
        self.B = (self.f, 2 * (3 - self.x) + self.c)
        self.C = (self.f, self.h + 1 - 2 * self.c)
        self.AC = (self.f, 2 * ax + 1 - self.c)

    def H(self, d):
        return (self.f, (self.h + d) % 8)

    def Y(self, d):
        return (4 * self.z + (self.y + d) % 4, self.h)

    def Z(self, d):
        return (4 * ((self.z + d) % 4) + self.y, self.h)


def quarter(h):
    x = h // 2
    return 2 * ((x + x // 2) % 2) + h % 2


class Comm:
    def __init__(self, ssem, rsem, lsem):
        self.ssem, self.rsem, self.lsem = ssem, rsem, lsem
        self.k = 0
        self.lk = 0
        self.sent = []

    def send(self, src, dst, dev):
        c = pltpu.make_async_remote_copy(src_ref=src, dst_ref=dst, send_sem=self.ssem.at[self.k],
                                         recv_sem=self.rsem.at[self.k], device_id=dev, device_id_type=MESH)
        self.k += 1
        c.start()
        self.sent.append(c)
        return c

    def local(self, src, dst):
        c = pltpu.make_async_copy(src, dst, self.lsem.at[self.lk])
        self.lk += 1
        c.start()
        return c

    def finish(self):
        for c in self.sent:
            c.wait_send()


class Part(Comm):
    def __init__(self, cm):
        self.cm = cm
        self.sent = []

    def send(self, src, dst, dev):
        c = self.cm.send(src, dst, dev)
        self.sent.append(self.cm.sent.pop())
        return c

    def local(self, src, dst):
        return self.cm.local(src, dst)


def barrier(devs):
    b = pltpu.get_barrier_semaphore()
    for d in devs:
        pl.semaphore_signal(b, inc=1, device_id=d, device_id_type=MESH)
    pl.semaphore_wait(b, len(devs))


def run(*gens):
    live = []
    for g in gens:
        t = next(g, None)
        if t is not None:
            live.append([t, g])
    while live:
        e = min(live, key=lambda v: v[0])
        t = next(e[1], None)
        if t is None:
            live.remove(e)
        else:
            e[0] = t


def ring_ag(cm, own, blk, half, m, plus, minus, t0, u):
    lo, hi = (m + 3) % 4, (m + 1) % 4
    p0 = cm.send(own, blk(m), plus)
    m0 = cm.send(own, blk(m), minus)
    yield t0 + u
    p0.wait_recv()
    p1 = cm.send(half(lo, 0), half(lo, 0), plus)
    m0.wait_recv()
    m1 = cm.send(half(hi, 1), half(hi, 1), minus)
    yield t0 + 1.5 * u
    p1.wait_recv()
    m1.wait_recv()


def ring_direct(cm, own, blk, m, sides, t0, u):
    c = [cm.send(own, blk(m), v) for v in sides]
    yield t0 + u
    for v in c:
        v.wait_recv()


def plane_ag(cm, p, own, n_o, half, t0, u1, u2):
    if half is None:
        ya = ring_direct(cm, own(0), lambda i: n_o(p.z, i, 0), p.y, (p.Y(1), p.Y(-1), p.Y(2)), t0, u1)
        zb = ring_direct(cm, own(1), lambda i: n_o(i, p.y, 1), p.z, (p.Z(1), p.Z(-1), p.Z(2)), t0, u1)
    else:
        ya = ring_ag(cm, own(0), lambda i: n_o(p.z, i, 0), lambda i, s: half(n_o(p.z, i, 0), s), p.y, p.Y(1), p.Y(-1), t0, u1)
        zb = ring_ag(cm, own(1), lambda i: n_o(i, p.y, 1), lambda i, s: half(n_o(i, p.y, 1), s), p.z, p.Z(1), p.Z(-1), t0, u1)
    loc = [cm.local(own(k), n_o(p.z, p.y, k)) for k in range(2)]
    for t, _ in zip(ya, zb):
        yield t
    list(zb)
    for v in loc:
        v.wait()
    t1 = t0 + (u1 if half is None else 1.5 * u1 + 2.0)
    al, h2 = slice(None), lambda s: pl.ds(2 * s, 2)
    za = ring_ag(cm, n_o(p.z, al, 0), lambda i: n_o(i, al, 0), lambda i, s: n_o(i, h2(s), 0), p.z, p.Z(1), p.Z(-1), t1, u2)
    yb = ring_ag(cm, n_o(al, p.y, 1), lambda i: n_o(al, i, 1), lambda i, s: n_o(h2(s), i, 1), p.y, p.Y(1), p.Y(-1), t1, u2)
    for t, _ in zip(za, yb):
        yield t
    list(yb)


def ring_rs(cm, get, r1p, r1m, fp, fm, res, m, plus, minus, t0, t1):
    lo, hi, far = (m + 3) % 4, (m + 1) % 4, (m + 2) % 4
    hb = r1p.shape[-2]
    f0, f1 = (Ellipsis, pl.ds(0, hb), slice(None)), (Ellipsis, pl.ds(hb, hb), slice(None))
    p0 = cm.send(get(far, 0), r1p, plus)
    m0 = cm.send(get(far, 1), r1m, minus)
    p1 = cm.send(get(hi, 1), fp.at[f1], plus)
    m1 = cm.send(get(lo, 0), fm.at[f0], minus)
    yield t0
    p0.wait_recv()
    v = get(hi, 0)
    v[...] = r1p[...] + v[...]
    p2 = cm.send(v, fp.at[f0], plus)
    m0.wait_recv()
    v = get(lo, 1)
    v[...] = r1m[...] + v[...]
    m2 = cm.send(v, fm.at[f1], minus)
    yield t1
    p1.wait_recv()
    m1.wait_recv()
    p2.wait_recv()
    m2.wait_recv()
    res(0)[...] = (fp[f0] + fm[f0]) + get(m, 0)[...]
    res(1)[...] = (fp[f1] + fm[f1]) + get(m, 1)[...]


def ring_rs_direct(cm, get, r, res, m, sides, t0, u):
    c = [cm.send(get((m + k + 1) % 4), r.at[k], v) for k, v in enumerate(sides)]
    yield t0 + u
    for v in c:
        v.wait_recv()
    res[...] = (r[0] + r[1]) + (r[2] + get(m)[...])


def block(x, g, wg, wu, wd, o, wo, wq, x_o, q_o,
          xs, gb, nb, n, wgb, wub, wdb, wob, wqb, ov, a1, a2, y,
          r1, f1, r2, s2, xn, xr, nh, qk, xq, ssem, rsem, lsem):
    p = Pos()
    cm = Comm(ssem, rsem, lsem)
    barrier([p.H(k) for k in range(1, 8)] + [p.Y(k) for k in range(1, 4)] + [p.Z(k) for k in range(1, 4)])
    tb, dh = xs.shape[1:]
    ww = wgb.shape[2]
    d = n.shape[3]
    dc = d // 2
    hb = tb // 2
    qb = hb // 2
    al = slice(None)

    def dyn(i, m):
        return pl.ds(pl.multiple_of(i * m, m), m)

    def rows(q):
        return x.at[pl.ds(pl.multiple_of(1024 * q + tb * p.f, tb), tb), :]

    xin = []
    for k in range(1, 8):
        t = p.H(k)
        xin.append(cm.send(rows(quarter(t[1])), xs.at[p.h], t))
        xin.append(cm.send(g, gb.at[p.h], t))
    loc = [cm.local(rows(p.q), xs.at[p.h]), cm.local(g, gb.at[p.h])]

    cw = ((0, 512), (512, 256))

    def cols(w, j, k):
        return w.at[:, pl.ds(pl.multiple_of(ww * j + cw[k][0], 128), cw[k][1])]

    def part_of(b, h, k):
        return b.at[h, :, pl.ds(*cw[k])]

    def slot(b, h):
        return b.at[:, dyn(h % 4, dh)]

    down_in, late, got, own = [], [], [[], []], []
    cn = Part(cm)
    ready = [[], []]

    def weights():
        ws = ((wg, wgb), (wu, wub))
        fb, fa, f2_ = [[], []], [[], []], [[], []]
        opp = 2 * (3 - p.A[1] // 2) + p.c

        def fan(k, to_b, to_a):
            for w, wb in ws:
                dst = part_of(wb, p.h, k)
                if to_b:
                    fb[k].append(cm.send(cols(w, 1 - p.j, k), dst, p.B))
                if to_a:
                    fa[k].append(cm.send(cols(w, p.j, k), dst, p.A))
                    ready[k].append(cm.send(cols(w, p.j, k), dst, p.C).wait_recv)
                    ready[k].append(cm.local(cols(w, p.j, k), dst).wait)

        def take(c, wb, h, k, onward):
            c.wait_recv()
            v = part_of(wb, h, k)
            if onward:
                f2_[k].append(cm.send(v, v, p.A))
            ready[k].append(cm.send(v, v, p.C).wait_recv)

        fan(0, True, True)
        fan(1, True, False)
        own.append(cm.local(o.at[pl.ds(pl.multiple_of(1024 * p.q, 1024), 1024), :], ov))
        for w, wb in ((wd, wdb), (wo, wob)):
            own.append(cm.local(w, slot(wb, p.h)))
        own.append(cm.local(wq, wqb.at[p.h]))
        for k in range(2):
            yield 14.0 + 8.0 * k
            take(fb[0][k], ws[k][1], p.B[1], 0, True)
            take(fa[0][k], ws[k][1], p.A[1], 0, False)
        fan(1, False, True)
        yield 31.0
        for k in range(2):
            take(fb[1][k], ws[k][1], p.B[1], 1, True)
        hk = wd.shape[0] // 2
        down_in.append((cm.send(wo, slot(wob, p.h), p.A), slot(wob, p.A[1])))
        late.append(cm.send(wo, slot(wob, p.h), p.C))
        for r in range(2):
            down_in.append((cm.send(wd.at[pl.ds(hk * r, hk), :], slot(wdb, p.h).at[pl.ds(hk * r, hk), :], p.A),
                            slot(wdb, p.A[1]).at[pl.ds(hk * r, hk), :]))
        late.append(cm.send(wd, slot(wdb, p.h), p.C))
        for k in range(2):
            yield 34.0 + 7.0 * k
            take(f2_[0][k], ws[k][1], opp, 0, False)
        yield 49.0
        for k in range(2):
            take(fa[1][k], ws[k][1], p.A[1], 1, False)
        for k in range(2):
            yield 56.0 + 4.5 * k
            take(f2_[1][k], ws[k][1], opp, 1, False)

    def tokens():
        yield 5.0
        for v in xin:
            v.wait_recv()
        for v in loc:
            v.wait()
        ss = jnp.zeros((tb, 1), F32)
        for k in range(8):
            v = xs[k].astype(F32)
            ss = ss + jnp.sum(v * v, axis=-1, keepdims=True)
        r = lax.rsqrt(ss / float(d) + EPS)
        for k in range(8):
            for i in range(dh // 128):
                ls = slice(128 * i, 128 * (i + 1))
                nb[:, dh * k + 128 * i:dh * k + 128 * (i + 1)] = (xs[k, :, ls].astype(F32) * r * gb[k, i:i + 1, :]).astype(BF)
        part = (pl.ds(0, dc), pl.ds(dc, dc))
        yield from plane_ag(cn, p, lambda k: nb.at[:, part[k]], lambda zi, yi, k: n.at[zi, yi, :, part[k]],
                            lambda v, s: v.at[pl.ds(hb * s, hb), :], 13.0, 6.0, 16.0)

    tn = 256

    def gate_up(k, b):
        s, zh = b // 2, b % 2

        def step(t, carry):
            v = n[2 * zh:2 * zh + 2, :, hb * s:hb * (s + 1), :].reshape(8 * hb, d)
            cs = pl.ds(pl.multiple_of(cw[k][0] + t * tn, tn), tn)
            gt = _dot(v, wgb[:, :, cs].reshape(d, tn))
            up = _dot(v, wub[:, :, cs].reshape(d, tn))
            a1[b, :, cs] = (jax.nn.silu(gt) * up).astype(BF)
            return carry

        lax.fori_loop(0, cw[k][1] // tn, step, 0)
        got[k].append(cm.send(part_of(a1, b, k), part_of(a2, b, k), p.B))

    def first():
        yield from tokens()
        yield 47.5
        for wait in ready[0]:
            wait()
        for b in range(4):
            gate_up(0, b)
            yield 51.0 + 2.0 * b

    run(first(), weights())
    for wait in ready[1]:
        wait()
    for b in range(4):
        gate_up(1, b)
    for v in own:
        v.wait()
    cn.finish()

    qc = []
    m = p.x
    lo, hi, far = (m + 3) % 4, (m + 1) % 4, (m + 2) % 4

    def qweights():
        def blk(i):
            return wqb.at[2 * i + p.c]

        hr = wq.shape[0] // 2

        def half(i, s):
            return wqb.at[2 * i + p.c, pl.ds(hr * s, hr), :]

        p0 = cm.send(wq, blk(m), p.H(2))
        m0 = cm.send(wq, blk(m), p.H(-2))
        qc.append(cm.send(wq, blk(m), p.C))
        yield 104.0
        p0.wait_recv()
        p1 = cm.send(half(lo, 0), half(lo, 0), p.H(2))
        qc.append(cm.send(blk(lo), blk(lo), p.C))
        m0.wait_recv()
        m1 = cm.send(half(hi, 1), half(hi, 1), p.H(-2))
        qc.append(cm.send(blk(hi), blk(hi), p.C))
        yield 111.5
        p1.wait_recv()
        m1.wait_recv()
        qc.append(cm.send(blk(far), blk(far), p.C))
        yield 115.0
        for v in qc:
            v.wait_recv()

    w3 = wdb.shape[1] // 2
    w4 = w3 // 2
    odd = p.x % 2
    xex = []

    def down(b, e):
        s, zh = b // 2, b % 2
        if e == 0:
            for k in range(2):
                got[k][b].wait_recv()
        base = w3 * (odd if e == 0 else 1 - odd)

        def step(t, carry):
            cs = pl.ds(pl.multiple_of(base + t * tn, tn), tn)
            ob = ov[512 * zh:512 * (zh + 1), :].reshape(8, tb, -1)[:, hb * s:hb * (s + 1), :].reshape(8 * hb, -1)
            v = (_dot(a1[b], wdb[dyn(p.j, ww), cs]) + _dot(a2[b], wdb[dyn(1 - p.j, ww), cs]) + _dot(ob, wob[:, cs]))
            y[s, 2 * zh:2 * zh + 2, :, :, pl.ds(pl.multiple_of(w3 * e + t * tn, tn), tn)] = v.reshape(2, 4, hb, tn)
            return carry

        lax.fori_loop(0, w3 // tn, step, 0, unroll=True)

    def rr(k):
        return pl.ds(qb * k, qb)

    ay, az = (p.y, p.Y(1), p.Y(-1)), (p.z, p.Z(1), p.Z(-1))

    def scatter(s, e, t0, t1, t2):
        ca, cb = pl.ds(w3 * e, w4), pl.ds(w3 * e + w4, w4)

        def both(get_a, get_b, r, f, res_a, res_b, ax_a, ax_b):
            ga = ring_rs(cm, get_a, r.at[s, e, 0], r.at[s, e, 1], f.at[s, e, 0], f.at[s, e, 1], res_a, *ax_a, t0, t1)
            gb_ = ring_rs(cm, get_b, r.at[s, e, 2], r.at[s, e, 3], f.at[s, e, 2], f.at[s, e, 3], res_b, *ax_b, t0, t1)
            for q, _ in zip(ga, gb_):
                yield q
            list(gb_)

        yield from both(lambda i, k: y.at[s, :, i, rr(k), ca], lambda i, k: y.at[s, i, :, rr(k), cb], r1, f1,
                        lambda k: y.at[s, :, p.y, rr(k), ca], lambda k: y.at[s, p.z, :, rr(k), cb], ay, az)
        y3, z3 = [p.Y(k) for k in (1, 2, 3)], [p.Z(k) for k in (1, 2, 3)]
        ga = ring_rs_direct(cm, lambda i: y.at[s, i, p.y, :, ca], r2.at[s, e, 0], s2.at[s, e, 0], p.z, z3, t2, 0.0)
        gb_ = ring_rs_direct(cm, lambda i: y.at[s, p.z, i, :, cb], r2.at[s, e, 1], s2.at[s, e, 1], p.y, y3, t2, 0.0)
        for q, _ in zip(ga, gb_):
            yield q
        list(gb_)

    def weights2():
        for k, (v, sl) in enumerate(down_in):
            yield (66.0, 74.0, 86.3)[k]
            v.wait_recv()
            late.append(cm.send(sl, sl, p.C))

    def own_part(s, t0, t):
        yield t0 - 2.0
        if s == 0:
            for v in late[:2]:
                v.wait_recv()
            del late[:2]
        down(2 * s, 0)
        yield t0
        down(2 * s + 1, 0)
        yield from scatter(s, 0, *t)

    def chain(s, t0, dt, t):
        yield t0 - 2.0
        if s == 0:
            for v in late:
                v.wait_recv()
        down(2 * s, 1)
        down(2 * s + 1, 1)
        yield from scatter(s, 1, *t)
        for _ in owns[s]:
            pass
        t = t0 + 14.5 + dt
        rs = pl.ds(hb * s, hb)
        for e in range(2):
            for k in range(2):
                i = 2 * (odd if e == 0 else 1 - odd) + k
                xn[s, :, dyn(i, dh)] = (xs[4 * p.j + i, rs, :].astype(F32) + s2[s, e, k]).astype(BF)
        ex = cm.send(xn.at[s, dyn(1 - p.j, qb), :], xr.at[s], p.B)
        for v in (p.A, p.C, p.AC):
            xex.append(cm.send(xn.at[s, :, dyn(v[1] % 4, dh)], xq.at[p.q, rs, :], v).wait_recv)
        xex.append(cm.local(xn.at[s, :, dyn(p.h % 4, dh)], xq.at[p.q, rs, :]).wait)
        mine = xn[s, dyn(p.j, qb), :].astype(F32)
        yield t + 2.0
        ex.wait_recv()
        oth = xr[s].astype(F32)
        ss = jnp.sum(mine * mine, axis=-1, keepdims=True) + jnp.sum(oth * oth, axis=-1, keepdims=True)
        r = lax.rsqrt(ss / float(d) + EPS)
        ng = dh // 128
        for k in range(4):
            for i in range(ng):
                cs = slice(dh * k + 128 * i, dh * k + 128 * (i + 1))
                gs = slice(ng + i, ng + i + 1)
                nh[s, p.j, :, cs] = (mine[:, cs] * r * gb[4 * p.j + k, gs, :]).astype(BF)
                nh[s, 1 - p.j, :, cs] = (oth[:, cs] * r * gb[4 * (1 - p.j) + k, gs, :]).astype(BF)
        part = (pl.ds(0, dc), pl.ds(dc, dc))
        n1 = n.at[:, :, pl.ds(hb * s, qb), :]
        yield from plane_ag(cm, p, lambda k: nh.at[s, k], lambda zi, yi, k: n1.at[zi, yi, :, part[k]],
                            None, t + 3.0, 3.0, 6.0)
        yield t + 15.5

        if s == 0:
            for _ in qw:
                pass

        def proj(t_, carry):
            cs = dyn(t_, tn)
            qk[s, :, :, cs] = _dot(n[:, :, hb * s:hb * s + qb, :].reshape(16 * qb, d), wqb[:, :, cs].reshape(d, tn)).astype(BF).reshape(16, qb, tn)
            return carry

        lax.fori_loop(0, wq.shape[1] // tn, proj, 0, unroll=True)

        def blk(xx):
            h = 2 * xx + p.c
            return q_o.at[quarter(h), :, s, h // 4]

        def half(xx, k):
            h = 2 * xx + p.c
            return q_o.at[quarter(h), pl.ds(8 * k, 8), s, h // 4]

        own = cm.local(qk.at[s], blk(m))
        p0 = cm.send(qk.at[s], blk(m), p.H(2))
        m0 = cm.send(qk.at[s], blk(m), p.H(-2))
        c = [cm.send(qk.at[s], blk(m), p.C)]
        yield t + 26.0 - 0.4 * dt
        p0.wait_recv()
        p1 = cm.send(half(lo, 0), half(lo, 0), p.H(2))
        m0.wait_recv()
        m1 = cm.send(half(hi, 1), half(hi, 1), p.H(-2))
        for b in (blk(lo), blk(hi)):
            c.append(cm.send(b, b, p.C))
        yield t + 32.0 - 0.4 * dt
        p1.wait_recv()
        c.append(cm.send(half(far, 0), half(far, 0), p.C))
        m1.wait_recv()
        c.append(cm.send(half(far, 1), half(far, 1), p.C))
        yield t + 36.0 + 0.5 * dt
        own.wait()
        for v in c:
            v.wait_recv()

    def resid():
        yield 130.5
        for wait in xex:
            wait()
        yield from plane_ag(cm, p, lambda k: xq.at[pl.ds(2 * k, 2)], lambda zi, yi, k: x_o.at[pl.ds(2 * k, 2), zi, yi],
                            None, 131.5, 4.0, 6.5)

    def qrest():
        yield 89.0
        yield next(qw)
        yield from qw

    qw = qweights()
    owns = [own_part(0, 75.0, (81.0, 86.0, 90.0)), own_part(1, 81.0, (87.0, 100.5, 104.0))]
    run(qrest(), weights2(), owns[0], owns[1], chain(0, 92.0, 0.0, (97.3, 102.3, 106.3)), chain(1, 94.6, 4.0, (99.9, 104.9, 108.9)), resid())
    cm.finish()


def solution(mesh):
    def body(x, g1, g2, w_gate, w_up, w_down, o, w_o, w_qkv):
        t, dh = x.shape
        d = dh * 8
        ff = w_gate.shape[1]
        tq = t // 4
        tb = tq // 16
        fh = ff // 2
        hb, qb, w2, nq = tb // 2, tb // 4, d // 4, w_qkv.shape[1]
        g = jnp.concatenate([g1, g2]).reshape(2 * dh // 128, 128)
        bf, f32 = (lambda *v: pltpu.VMEM(v, BF)), (lambda *v: pltpu.VMEM(v, F32))
        ns = 232
        xo, qo = pl.pallas_call(
            block,
            out_shape=[jax.ShapeDtypeStruct((4, 4, 4, tb, dh), BF), jax.ShapeDtypeStruct((4, 16, 2, 2, qb, nq), BF)],
            in_specs=[HB] * 8,
            out_specs=[ANY] * 2,
            scratch_shapes=[
                bf(8, tb, dh), f32(8, 2 * dh // 128, 128), bf(tb, d), bf(4, 4, tb, d), bf(8, dh, fh), bf(8, dh, fh),
                bf(ff, d // 2), bf(w_o.shape[0], d // 2), bf(8, dh, nq), bf(tq, w_o.shape[0]),
                bf(4, tq // 4, fh), bf(4, tq // 4, fh), f32(2, 4, 4, hb, d // 2),
                f32(2, 2, 4, 4, qb, w2 // 2), f32(2, 2, 4, 4, hb, w2 // 2), f32(2, 2, 2, 3, hb, w2 // 2),
                f32(2, 2, 2, hb, w2 // 2),
                bf(2, hb, d // 2), bf(2, qb, d // 2), bf(2, 2, qb, d // 2), bf(2, 16, qb, nq),
                bf(4, tb, dh),
                pltpu.SemaphoreType.DMA((ns,)), pltpu.SemaphoreType.DMA((ns,)), pltpu.SemaphoreType.DMA((28,))],
            compiler_params=pltpu.CompilerParams(collective_id=1, has_side_effects=True,
                                                 vmem_limit_bytes=VLIM),
            name='block',
        )(x, g, w_gate, w_up, w_down, o, w_o, w_qkv)
        return xo.reshape(t, dh), qo.reshape(t, -1)

    in_specs = (P(None, 'h'), P('h'), P('h'), P('h', 'f'), P('h', 'f'), P('f', 'h'),
                P(None, 'f'), P('f', 'h'), P('h', 'f'))
    return jax.shard_map(body, mesh=mesh, in_specs=in_specs,
                         out_specs=(P(None, 'h'), P(None, 'f')), check_vma=False)
```
